16 devices in a mesh: dp: 4 (over z, y), tp: 4 (over x, core).
Axes of the slice: x: 2, y: 2, z: 2, core: 2. Of those that a mesh axis runs over, the one named last changes fastest.
Arguments:
- token_ids: int32 [4, 256], P('dp'), parts along dimension 0
- embed_table: bfloat16 [16384, 2048], P('tp')
- emb_gain: float32 [2048], replicated
- emb_bias: float32 [2048], replicated
- ln1_gain: float32 [2048], replicated
- ln1_bias: float32 [2048], replicated
- w_qkv: bfloat16 [2048, 16, 3, 128], P(None, 'tp')
- b_qkv: float32 [16, 3, 128], P('tp')
- w_dense: bfloat16 [2048, 2048], P('tp')
- b_dense: float32 [2048], replicated
- ln2_gain: float32 [2048], replicated
- ln2_bias: float32 [2048], replicated
- w_fc1: bfloat16 [2048, 8192], P(None, 'tp')
- b_fc1: float32 [8192], P('tp')
- w_fc2: bfloat16 [8192, 2048], P('tp')
- b_fc2: float32 [2048], replicated
- d_out: bfloat16 [4, 256, 2048], P('dp', 'tp'), parts along dimension 0
Outputs:
- output 1: bfloat16 [4, 256, 2048], P('dp', 'tp'), parts along dimension 0
- output 2: float32 [65536, 2048], P(('dp', 'tp')), parts along dimension 0
- output 3: float32 [8192], P('dp'), parts along dimension 0
- output 4: float32 [8192], P('dp'), parts along dimension 0
- output 5: float32 [8192], P('dp'), parts along dimension 0
- output 6: float32 [8192], P('dp'), parts along dimension 0
- output 7: bfloat16 [8192, 16, 3, 128], P('dp', 'tp'), parts along dimension 0
- output 8: float32 [64, 3, 128], P(('dp', 'tp')), parts along dimension 0
- output 9: bfloat16 [8192, 2048], P(('dp', 'tp')), parts along dimension 0
- output 10: float32 [8192], P('dp'), parts along dimension 0
- output 11: float32 [8192], P('dp'), parts along dimension 0
- output 12: float32 [8192], P('dp'), parts along dimension 0
- output 13: bfloat16 [8192, 8192], P('dp', 'tp'), parts along dimension 0
- output 14: float32 [32768], P(('dp', 'tp')), parts along dimension 0
- output 15: bfloat16 [32768, 2048], P(('dp', 'tp')), parts along dimension 0
- output 16: float32 [8192], P('dp'), parts along dimension 0
There are 4 independent parts. The reference program is written for one: setup_inputs(seed, part) draws one part's arguments, and reference() takes and returns one part's arrays. A program takes and returns all parts, laid end to end along the dimension named above; an argument that names none is the same for every part.
All inputs are finite; a program needn't handle non-finite values.
Results may differ from the reference program's by a relative error of at most 0.02.
Values are sent between devices in bfloat16 or wider.
A program may use at most 1 GiB of HBM per device.

```python
import jax
import jax.numpy as jnp
from jax import lax

BATCH = 1
SEQ = 256
D_MODEL = 2048
HEADS = 16
VOCAB = 16384

HEAD_DIM = D_MODEL // HEADS
FFN = 4 * D_MODEL
EPS = 1e-5


def draw_ids(id_key):
    key_a, key_b, key_c, key_d = jax.random.split(id_key, 4)
    shape_ids = (BATCH, SEQ)
    upper_one = jax.random.randint(key_a, shape_ids, 1, VOCAB + 1)
    upper_two = jax.random.randint(key_b, shape_ids, 1, upper_one + 1)
    skewed = jax.random.randint(key_c, shape_ids, 0, upper_two)
    positions = jnp.arange(SEQ)
    stripe_lo = (positions // 4) * 4 * VOCAB // SEQ
    stripe_hi = (positions // 4 + 1) * 4 * VOCAB // SEQ
    spread = jax.random.randint(key_d, shape_ids, stripe_lo, stripe_hi)
    return jnp.where(positions % 4 == 0, spread, skewed).astype(jnp.int32)


def setup_inputs(seed: int = 0, part: int = 0) -> dict:
    root_key = jax.random.key(seed)
    part_key = jax.random.fold_in(root_key, part)
    key_list = jax.random.split(root_key, 15)
    id_key, grad_key = jax.random.split(part_key)

    def draw_normal(slot_num, shape_out, scale_by):
        return scale_by * jax.random.normal(key_list[slot_num], shape_out, jnp.float32)

    scale_in = D_MODEL ** -0.5
    scale_ff = FFN ** -0.5
    return {
        'token_ids': draw_ids(id_key),
        'embed_table': draw_normal(0, (VOCAB, D_MODEL), 1.0).astype(jnp.bfloat16),
        'emb_gain': 1.0 + draw_normal(1, (D_MODEL,), 0.25),
        'emb_bias': draw_normal(2, (D_MODEL,), 0.25),
        'ln1_gain': 1.0 + draw_normal(3, (D_MODEL,), 0.25),
        'ln1_bias': draw_normal(4, (D_MODEL,), 0.25),
        'w_qkv': draw_normal(5, (D_MODEL, HEADS, 3, HEAD_DIM), scale_in).astype(jnp.bfloat16),
        'b_qkv': draw_normal(6, (HEADS, 3, HEAD_DIM), 0.3),
        'w_dense': draw_normal(7, (D_MODEL, D_MODEL), scale_in).astype(jnp.bfloat16),
        'b_dense': draw_normal(8, (D_MODEL,), 0.3),
        'ln2_gain': 1.0 + draw_normal(9, (D_MODEL,), 0.25),
        'ln2_bias': draw_normal(10, (D_MODEL,), 0.25),
        'w_fc1': draw_normal(11, (D_MODEL, FFN), scale_in).astype(jnp.bfloat16),
        'b_fc1': draw_normal(12, (FFN,), 0.3),
        'w_fc2': draw_normal(13, (FFN, D_MODEL), scale_ff).astype(jnp.bfloat16),
        'b_fc2': draw_normal(14, (D_MODEL,), 0.3),
        'd_out': jax.random.normal(grad_key, (BATCH, SEQ, D_MODEL), jnp.float32).astype(jnp.bfloat16),
    }


def to_bf16(values):
    return values.astype(jnp.bfloat16).astype(jnp.float32)


def layer_norm(values, gain_vec, bias_vec):
    centered = values - jnp.mean(values, axis=-1, keepdims=True)
    var_val = jnp.mean(centered * centered, axis=-1, keepdims=True)
    return centered * lax.rsqrt(var_val + EPS) * gain_vec + bias_vec


def alibi_slopes():
    closest = 2 ** (HEADS.bit_length() - 1)
    slope_base = 2.0 ** (-8.0 / closest)
    extra_base = 2.0 ** (-4.0 / closest)
    slopes = [slope_base ** exponent for exponent in range(1, closest + 1)]
    slopes = slopes + [extra_base ** exponent for exponent in range(1, 2 * (HEADS - closest), 2)]
    return jnp.array(slopes, dtype=jnp.float32)


def seq_forward(x_seq, params):
    (emb_gain, emb_bias, ln1_gain, ln1_bias, w_qkv, b_qkv, w_dense, b_dense,
     ln2_gain, ln2_bias, w_fc1, b_fc1, w_fc2, b_fc2) = params
    embedded = to_bf16(layer_norm(x_seq, emb_gain, emb_bias))
    h_one = to_bf16(layer_norm(embedded, ln1_gain, ln1_bias))
    qkv_all = to_bf16(jnp.einsum('sd,dhce->shce', h_one, w_qkv) + b_qkv)
    positions = jnp.arange(SEQ)
    rel_pos = (positions[None, :] - positions[:, None]).astype(jnp.float32)
    causal = positions[None, :] <= positions[:, None]
    scores = jnp.einsum('qhe,khe->hqk', qkv_all[:, :, 0], qkv_all[:, :, 1]) * HEAD_DIM ** -0.5
    scores = jnp.where(causal, scores + alibi_slopes()[:, None, None] * rel_pos, -1e30)
    prob_bf = to_bf16(jax.nn.softmax(scores, axis=-1))
    context = to_bf16(jnp.einsum('hqk,khe->qhe', prob_bf, qkv_all[:, :, 2])).reshape(SEQ, D_MODEL)
    r_one = to_bf16(embedded + jnp.dot(context, w_dense, preferred_element_type=jnp.float32) + b_dense)
    h_two = to_bf16(layer_norm(r_one, ln2_gain, ln2_bias))
    gelu_out = to_bf16(jax.nn.gelu(jnp.dot(h_two, w_fc1, preferred_element_type=jnp.float32) + b_fc1, approximate=True))
    return to_bf16(r_one + jnp.dot(gelu_out, w_fc2, preferred_element_type=jnp.float32) + b_fc2)


def reference(token_ids, embed_table, emb_gain, emb_bias, ln1_gain, ln1_bias, w_qkv, b_qkv,
              w_dense, b_dense, ln2_gain, ln2_bias, w_fc1, b_fc1, w_fc2, b_fc2, d_out):
    params = tuple(weight.astype(jnp.float32) for weight in (
        emb_gain, emb_bias, ln1_gain, ln1_bias, w_qkv, b_qkv, w_dense, b_dense,
        ln2_gain, ln2_bias, w_fc1, b_fc1, w_fc2, b_fc2))
    x_zero = jnp.take(embed_table, token_ids, axis=0).astype(jnp.float32)

    def seq_step(grad_sum, step_in):
        x_seq, dy_seq = step_in
        y_seq, pull_back = jax.vjp(seq_forward, x_seq, params)
        dx_seq, d_params = pull_back(dy_seq.astype(jnp.float32))
        grad_sum = jax.tree.map(jnp.add, grad_sum, d_params)
        return grad_sum, (y_seq.astype(jnp.bfloat16), dx_seq.astype(jnp.bfloat16))

    grad_zero = jax.tree.map(jnp.zeros_like, params)
    grad_total, (y_out, dx_zero) = lax.scan(seq_step, grad_zero, (x_zero, d_out))
    d_table = jax.ops.segment_sum(dx_zero.astype(jnp.float32).reshape(BATCH * SEQ, D_MODEL),
                                  token_ids.reshape(BATCH * SEQ), num_segments=VOCAB)
    (d_emb_gain, d_emb_bias, d_ln1_gain, d_ln1_bias, d_w_qkv, d_b_qkv, d_w_dense, d_b_dense,
     d_ln2_gain, d_ln2_bias, d_w_fc1, d_b_fc1, d_w_fc2, d_b_fc2) = grad_total
    return (y_out, d_table, d_emb_gain, d_emb_bias, d_ln1_gain, d_ln1_bias,
            d_w_qkv.astype(jnp.bfloat16), d_b_qkv, d_w_dense.astype(jnp.bfloat16), d_b_dense,
            d_ln2_gain, d_ln2_bias, d_w_fc1.astype(jnp.bfloat16), d_b_fc1,
            d_w_fc2.astype(jnp.bfloat16), d_b_fc2)
```

```python
import functools
import jax
import jax.numpy as jnp
from jax import lax
from jax.experimental import pallas as pl
from jax.experimental.pallas import tpu as pltpu
from jax.sharding import PartitionSpec as P

EPS = 1e-5
F32 = jnp.float32
BF16 = jnp.bfloat16
VMEM = pltpu.VMEM
ANY = pl.ANY
MAX_VMEM = 67_043_328
NT_DIMS = (((1,), (1,)), ((), ()))
TN_DIMS = (((0,), (0,)), ((), ()))
GELU_A = 0.7978845608028654
GELU_B = 0.044715


def alibi_slopes(head_count):
    closest = 2 ** (head_count.bit_length() - 1)
    slope_base = 2.0 ** (-8.0 / closest)
    extra_base = 2.0 ** (-4.0 / closest)
    slopes = [slope_base ** exponent for exponent in range(1, closest + 1)]
    return slopes + [extra_base ** exponent for exponent in range(1, 2 * (head_count - closest), 2)]


def dot_nn(lhs, rhs):
    return jnp.dot(lhs, rhs, preferred_element_type=F32)


def dot_nt(lhs, rhs):
    return lax.dot_general(lhs, rhs, NT_DIMS, preferred_element_type=F32)


def dot_tn(lhs, rhs):
    return lax.dot_general(lhs, rhs, TN_DIMS, preferred_element_type=F32)


def normalize(values):
    centered = values - jnp.mean(values, axis=-1, keepdims=True)
    inv_std = lax.rsqrt(jnp.mean(centered * centered, axis=-1, keepdims=True) + EPS)
    return centered * inv_std, inv_std


def norm_backward(d_norm, x_hat, inv_std, gain_vec):
    d_hat = d_norm * gain_vec
    return inv_std * (d_hat - jnp.mean(d_hat, axis=-1, keepdims=True)
                      - x_hat * jnp.mean(d_hat * x_hat, axis=-1, keepdims=True))


def gather_kernel(ids_smem, ids_vmem, table, out, stage, sem):
    tokens = ids_smem.shape[1]
    vocab_rows = table.shape[0]
    base = lax.axis_index('tp') * vocab_rows
    group = 32

    def copy_of(token):
        row = jnp.clip(ids_smem[0, token] - base, 0, vocab_rows - 1)
        first = pl.multiple_of((row // 8) * 8, 8)
        return pltpu.make_async_copy(table.at[pl.ds(first, 8), :],
                                     stage.at[pl.ds(pl.multiple_of(token * 8, 8), 8), :], sem)

    @pl.loop(0, tokens)
    def _(token):
        copy_of(token).start()

    pltpu.make_async_copy(table.at[pl.ds(0, tokens * 8), :], stage, sem).wait()

    local = ids_vmem[...] - base
    inside = jnp.where(local >= 0, 1, 0) * jnp.where(local < vocab_rows, 1, 0)
    sub = jnp.where(inside > 0, lax.rem(jnp.clip(local, 0, vocab_rows - 1), 8), -1)
    span = group * 8
    for block in range(tokens // group):
        sub_row = sub[:, block * group:(block + 1) * group]
        index = lax.broadcasted_iota(jnp.int32, (span, group), 0)
        lane = lax.broadcasted_iota(jnp.int32, (span, group), 1)
        pick = jnp.where(index == lane * 8 + sub_row, 1.0, 0.0)
        pick = jnp.where(sub_row >= 0, pick, 0.0).astype(BF16)
        rows = stage[block * span:(block + 1) * span, :]
        out[block * group:(block + 1) * group, :] = dot_tn(pick, rows).astype(BF16)


def gather_rows(token_ids, table):
    tokens, width = token_ids.shape[1], table.shape[1]
    return pl.pallas_call(
        gather_kernel,
        out_shape=jax.ShapeDtypeStruct((tokens, width), BF16),
        in_specs=[pl.BlockSpec(memory_space=pltpu.SMEM), pl.BlockSpec(memory_space=VMEM),
                  pl.BlockSpec(memory_space=ANY)],
        out_specs=pl.BlockSpec(memory_space=VMEM),
        scratch_shapes=[VMEM((tokens * 8, width), BF16), pltpu.SemaphoreType.DMA],
        compiler_params=pltpu.CompilerParams(vmem_limit_bytes=24 << 20),
        name='gather_rows',
    )(token_ids, token_ids, table)


CHUNKS = 2
AR_EMB, AR_DENSE, AR_DH2, AR_DH1 = range(4)
(ACC_EG, ACC_EB, ACC_L1G, ACC_L1B, ACC_BD, ACC_L2G, ACC_L2B, ACC_BF2) = range(8)
N_COPIES = 4 * CHUNKS * 4 + 3 + 3


def step_kernel(slopes, rows_in, w_qkv, w_dense, w_fc1, w_fc2, d_out,
                emb_gain, emb_bias, ln1_gain, ln1_bias, b_qkv, b_dense, ln2_gain, ln2_bias, b_fc1, b_fc2,
                o_h1, o_h2, o_ctx, o_gelu, o_dpre, o_dqkv, o_dy, o_dr1, o_dx, y_out, o_small, o_bfc1, o_bqkv,
                wraw, wtmp, wq, wd, w1, w2, part, din, summ, cross, dy, ypart, y_in, y_send, y_cross,
                emb, h1, qkv, ctx, r1, h2, gelu, dgelu, dpre, prob, dr1, d_kv, dqkv, dx, bq, acc,
                send_sem, recv_sem, load_sem, out_sem):
    tp = lax.axis_index('tp')
    core = lax.rem(tp, 2)
    chip = tp // 2
    partner = tp + 1 - 2 * core
    xpeer = lax.rem(tp + 2, 4)
    seq, width = emb.shape
    size = seq // CHUNKS
    half = size // 2
    heads, head_dim = b_qkv.shape[1], b_qkv.shape[2]
    scale = head_dim ** -0.5
    hidden = heads * head_dim
    block = seq // 4

    barrier = pltpu.get_barrier_semaphore()
    for peer in (partner, xpeer):
        pl.semaphore_signal(barrier, inc=1, device_id={'tp': peer}, device_id_type=pl.DeviceIdType.MESH)

    def load(src, dst, index):
        copy = pltpu.make_async_copy(src, dst, load_sem.at[index])
        copy.start()
        return copy

    load_rows = load(rows_in, part.at[AR_EMB], 0)
    my_block = pl.ds(pl.multiple_of(tp * block, block), block)
    load_dy = load(d_out, dy.at[my_block, :], 1)
    raw_rows = wraw.shape[1]
    raw_steps = w_qkv.shape[0] // raw_rows

    def load_raw(step):
        return pltpu.make_async_copy(w_qkv.at[pl.ds(pl.multiple_of(step * raw_rows, raw_rows), raw_rows)],
                                     wraw.at[lax.rem(step, 2)], load_sem.at[6 + lax.rem(step, 2)])

    load_raw(0).start()
    load_raw(1).start()
    load_wd = load(w_dense, wd, 2)
    load_w2 = load(w_fc2, w2, 3)
    load_w1 = load(w_fc1, w1, 4)

    count = [0]
    sends = []

    def remote(src, dst, peer):
        index = count[0]
        count[0] += 1
        copy = pltpu.make_async_remote_copy(src_ref=src, dst_ref=dst, send_sem=send_sem.at[index],
                                            recv_sem=recv_sem.at[index], device_id={'tp': peer},
                                            device_id_type=pl.DeviceIdType.MESH)
        sends.append(copy)
        return copy

    def at_row(start, length):
        return pl.ds(pl.multiple_of(start, half), length)

    def make_reduce(which, chunk):
        base = chunk * size
        mine, other = at_row(base + core * half, half), at_row(base + (1 - core) * half, half)
        local_in = din.at[which, pl.ds(chunk * half, half), :]
        first = remote(part.at[which, other, :], local_in, partner)
        across = remote(summ.at[which, mine, :], cross.at[which, mine, :], xpeer)
        share = remote(summ.at[which, mine, :], summ.at[which, mine, :], partner)
        forward = remote(cross.at[which, mine, :], cross.at[which, mine, :], partner)

        def middle():
            first.wait_recv()

            @pl.loop(0, half // 16)
            def _(i):
                rows = pl.ds(pl.multiple_of(base + core * half + i * 16, 16), 16)
                got = din[which, pl.ds(pl.multiple_of(chunk * half + i * 16, 16), 16), :]
                summ[which, rows, :] = (part[which, rows, :].astype(F32) + got.astype(F32)).astype(BF16)

            across.start()
            share.start()

        def pass_on():
            across.wait_recv()
            forward.start()

        def finish():
            share.wait_recv()
            forward.wait_recv()

        return first.start, middle, pass_on, finish

    reduces = {(w, c): make_reduce(w, c) for w in range(4) for c in range(CHUNKS)}

    def ar(which, chunk, stage):
        reduces[which, chunk][stage]()

    dy_across = remote(dy.at[my_block, :], dy.at[my_block, :], xpeer)
    dy_share = remote(dy.at[my_block, :], dy.at[my_block, :], partner)
    peer_block = pl.ds(pl.multiple_of(xpeer * block, block), block)
    dy_forward = remote(dy.at[peer_block, :], dy.at[peer_block, :], partner)

    partner_block = pl.ds(pl.multiple_of(partner * block, block), block)
    far = 2 * (1 - chip) + 1 - core
    far_block = pl.ds(pl.multiple_of(far * block, block), block)
    y_near = remote(ypart.at[partner_block, :], y_in.at[0], partner)
    y_far = remote(ypart.at[far_block, :], y_in.at[1], partner)
    y_over = remote(y_send, y_cross, xpeer)

    outs = []

    def put(src, dst):
        copy = pltpu.make_async_copy(src, dst, out_sem.at[len(outs)])
        copy.start()
        outs.append(copy)

    def row_loop(chunk, body, step=16):
        @pl.loop(0, size // step)
        def _(i):
            body(pl.ds(pl.multiple_of(chunk * size + i * step, step), step))

    def chunk_rows(chunk):
        return slice(chunk * size, (chunk + 1) * size)

    def col_loop(total, tile, body, first=0):
        @pl.loop(first, total // tile)
        def _(n):
            body(pl.ds(pl.multiple_of(n * tile, tile), tile))

    def accumulate(slot, values):
        acc[slot] += values[:8] + values[8:]

    def exchanged(which, rows):
        return summ[which, rows, :].astype(F32) + cross[which, rows, :].astype(F32)

    def unpack_qkv():
        pitch = wtmp.shape[0] // (3 * heads)
        for c in range(3):
            for h in range(heads):
                bq[0:1, c * hidden + h * head_dim:c * hidden + (h + 1) * head_dim] = b_qkv[c, h:h + 1, :]

        @pl.loop(0, raw_steps)
        def _(step):
            load_raw(step).wait()
            slot = lax.rem(step, 2)

            @pl.loop(0, raw_rows // 8)
            def _(i):
                for j in range(8):
                    for c in range(3):
                        d = i * 8 + j
                        wtmp[pl.ds(c * heads * pitch + d, heads, stride=pitch), :] = wraw[slot, d, c].astype(F32)

            @pl.when(step + 2 < raw_steps)
            def _():
                load_raw(step + 2).start()

            dst = pl.ds(pl.multiple_of(step * raw_rows, raw_rows), raw_rows)
            for c in range(3):
                for h in range(heads):
                    lo = c * hidden + h * head_dim
                    wq[dst, lo:lo + head_dim] = wtmp[(c * heads + h) * pitch:
                                                     (c * heads + h) * pitch + raw_rows, :].astype(BF16)

    def norm_first(chunk):
        def body(rows):
            x_hat, _ = normalize(exchanged(AR_EMB, rows))
            embedded = (x_hat * emb_gain[...] + emb_bias[...]).astype(BF16)
            emb[rows, :] = embedded
            e_hat, _ = normalize(embedded.astype(F32))
            h1[rows, :] = (e_hat * ln1_gain[...] + ln1_bias[...]).astype(BF16)

        row_loop(chunk, body)

    def project_qkv(chunk):
        rows = chunk_rows(chunk)

        def body(cols):
            qkv[rows, cols] = (dot_nn(h1[rows, :], wq[:, cols]) + bq[0:1, cols]).astype(BF16)

        col_loop(3 * hidden, 512, body)

    def head_cols(part_index, h):
        lo = part_index * hidden + h * head_dim
        return slice(lo, lo + head_dim)

    def attend(chunk):
        rows = chunk_rows(chunk)
        keys = (chunk + 1) * size
        row_id = lax.broadcasted_iota(jnp.int32, (size, keys), 0) + chunk * size
        col_id = lax.broadcasted_iota(jnp.int32, (size, keys), 1)
        rel = (col_id - row_id).astype(F32)
        for h in range(heads):
            slope = F32(slopes[3 * heads + h])
            for t in (2, 1, 0):
                slope = jnp.where(tp == t, F32(slopes[t * heads + h]), slope)
            scores = dot_nt(qkv[rows, head_cols(0, h)], qkv[0:keys, head_cols(1, h)]) * scale
            scores = jnp.where(col_id <= row_id, scores + slope * rel, -1e30)
            top = jnp.max(scores, axis=-1, keepdims=True)
            weight = jnp.exp(scores - top)
            p = weight / jnp.sum(weight, axis=-1, keepdims=True)
            prob[h, rows, 0:keys] = p
            ctx[rows, h * head_dim:(h + 1) * head_dim] = dot_nn(
                p.astype(BF16), qkv[0:keys, head_cols(2, h)]).astype(BF16)

    def project_dense(chunk):
        rows = chunk_rows(chunk)

        def body(cols):
            part[AR_DENSE, rows, cols] = dot_nn(ctx[rows, :], wd[:, cols]).astype(BF16)

        col_loop(width, 512, body)

    def norm_second(chunk):
        def body(rows):
            r_one = (emb[rows, :].astype(F32) + exchanged(AR_DENSE, rows) + b_dense[...]).astype(BF16)
            r1[rows, :] = r_one
            r_hat, _ = normalize(r_one.astype(F32))
            h2[rows, :] = (r_hat * ln2_gain[...] + ln2_bias[...]).astype(BF16)

        row_loop(chunk, body)

    def gelu_grad(first, last):
        @pl.loop(first, last)
        def _(n):
            cols = pl.ds(pl.multiple_of(n * 256, 256), 256)
            dgelu[:, cols] = dot_nt(dy[...], w2[cols, :])

    def widen(chunk):
        rows = chunk_rows(chunk)

        def body(cols):
            pre = dot_nn(h2[rows, :], w1[:, cols]) + b_fc1[0:1, cols]
            square = pre * pre
            bend = jnp.tanh(GELU_A * (pre + GELU_B * (pre * square)))
            gelu[rows, cols] = (0.5 * pre * (1.0 + bend)).astype(BF16)
            slope = 0.5 * (1.0 + bend) + 0.5 * pre * (1.0 - bend * bend) * (GELU_A * (1.0 + 3.0 * GELU_B * square))
            d_pre = dgelu[rows, cols] * slope
            dpre[rows, cols] = d_pre.astype(BF16)
            total = jnp.sum(d_pre, axis=0, keepdims=True)
            o_bfc1[0:1, cols] = total if chunk == 0 else o_bfc1[0:1, cols] + total

        col_loop(w1.shape[1], 256, body)

    def narrow_grad(chunk):
        rows = chunk_rows(chunk)

        def body(cols):
            part[AR_DH2, rows, cols] = dot_nt(dpre[rows, :], w1[cols, :]).astype(BF16)

        col_loop(width, 256, body)

    def narrow(first, last):
        @pl.loop(first, last)
        def _(n):
            cols = pl.ds(pl.multiple_of(n * 256, 256), 256)
            ypart[:, cols] = dot_nn(gelu[...], w2[:, cols]).astype(BF16)

    def y_middle():
        y_near.wait_recv()
        y_far.wait_recv()

        @pl.loop(0, block // 16)
        def _(i):
            rows = pl.ds(pl.multiple_of(i * 16, 16), 16)
            src = pl.ds(pl.multiple_of(xpeer * block + i * 16, 16), 16)
            y_send[rows, :] = (ypart[src, :].astype(F32) + y_in[1, rows, :].astype(F32)).astype(BF16)

        y_over.start()

    def y_finish():
        y_over.wait_recv()

        @pl.loop(0, block // 16)
        def _(i):
            rows = pl.ds(pl.multiple_of(i * 16, 16), 16)
            src = pl.ds(pl.multiple_of(tp * block + i * 16, 16), 16)
            total = ypart[src, :].astype(F32) + y_in[0, rows, :].astype(F32) + y_cross[rows, :].astype(F32)
            y_out[rows, :] = (r1[src, :].astype(F32) + total + b_fc2[...]).astype(BF16)

    def norm_second_grad(chunk):
        def body(rows):
            r_hat, inv = normalize(r1[rows, :].astype(F32))
            d_norm = exchanged(AR_DH2, rows)
            dy_rows = dy[rows, :].astype(F32)
            grad = dy_rows + norm_backward(d_norm, r_hat, inv, ln2_gain[...])
            dr1[rows, :] = grad.astype(BF16)
            accumulate(ACC_L2G, d_norm * r_hat)
            accumulate(ACC_L2B, d_norm)
            accumulate(ACC_BD, grad)
            accumulate(ACC_BF2, dy_rows)

        row_loop(chunk, body)

    def attend_grad(chunk):
        rows = chunk_rows(chunk)
        keys = (chunk + 1) * size
        old = chunk * size
        for h in range(heads):
            cols = slice(h * head_dim, (h + 1) * head_dim)
            d_ctx = dot_nt(dr1[rows, :], wd[cols, :]).astype(BF16)
            p = prob[h, rows, 0:keys]
            d_prob = dot_nt(d_ctx, qkv[0:keys, head_cols(2, h)])
            d_score = p * (d_prob - jnp.sum(d_prob * p, axis=-1, keepdims=True))
            d_score = (d_score * scale).astype(BF16)
            d_query = dot_nn(d_score, qkv[0:keys, head_cols(1, h)])
            dqkv[rows, head_cols(0, h)] = d_query.astype(BF16)
            total = jnp.sum(d_query, axis=0, keepdims=True)
            o_bqkv[0:1, head_cols(0, h)] = total if chunk == 0 else o_bqkv[0:1, head_cols(0, h)] + total
            for index, grad in ((0, dot_tn(d_score, qkv[rows, head_cols(0, h)])),
                                (1, dot_tn(p.astype(BF16), d_ctx))):
                if old:
                    d_kv[index, 0:old, cols] += grad[:old]
                d_kv[index, old:keys, cols] = grad[old:]

    def finish_kv():
        for index in range(2):
            lo = (index + 1) * hidden
            dqkv[:, lo:lo + hidden] = d_kv[index].astype(BF16)
            o_bqkv[0:1, lo:lo + hidden] = jnp.sum(d_kv[index], axis=0, keepdims=True)

    def qkv_grad(chunk):
        rows = chunk_rows(chunk)

        def body(cols):
            part[AR_DH1, rows, cols] = dot_nt(dqkv[rows, :], wq[cols, :]).astype(BF16)

        col_loop(width, 256, body)

    def norm_first_grad(chunk):
        def body(rows):
            e_hat, e_inv = normalize(emb[rows, :].astype(F32))
            d_norm = exchanged(AR_DH1, rows)
            grad = dr1[rows, :].astype(F32) + norm_backward(d_norm, e_hat, e_inv, ln1_gain[...])
            accumulate(ACC_L1G, d_norm * e_hat)
            accumulate(ACC_L1B, d_norm)
            x_hat, x_inv = normalize(exchanged(AR_EMB, rows))
            accumulate(ACC_EG, grad * x_hat)
            accumulate(ACC_EB, grad)
            dx[rows, :] = norm_backward(grad, x_hat, x_inv, emb_gain[...]).astype(BF16)

        row_loop(chunk, body)

    START, MIDDLE, PASS, FINISH = range(4)
    acc[...] = jnp.zeros_like(acc)
    load_rows.wait()
    pl.semaphore_wait(barrier, 2)
    ar(AR_EMB, 0, START)
    ar(AR_EMB, 1, START)
    ar(AR_EMB, 0, MIDDLE)
    ar(AR_EMB, 1, MIDDLE)
    load_dy.wait()
    dy_across.start()
    dy_share.start()
    unpack_qkv()
    load_wd.wait()
    ar(AR_EMB, 0, PASS)
    ar(AR_EMB, 0, FINISH)
    norm_first(0)
    project_qkv(0)
    ar(AR_EMB, 1, PASS)
    attend(0)
    project_dense(0)
    ar(AR_DENSE, 0, START)
    ar(AR_EMB, 1, FINISH)
    norm_first(1)
    put(h1, o_h1)
    ar(AR_DENSE, 0, MIDDLE)
    project_qkv(1)
    dy_across.wait_recv()
    dy_forward.start()
    attend(1)
    put(ctx, o_ctx)
    project_dense(1)
    ar(AR_DENSE, 1, START)
    dy_share.wait_recv()
    dy_forward.wait_recv()
    put(dy, o_dy)
    load_w2.wait()
    gelu_grad(0, 2)
    ar(AR_DENSE, 1, MIDDLE)
    gelu_grad(2, 8)
    ar(AR_DENSE, 0, PASS)
    ar(AR_DENSE, 0, FINISH)
    load_w1.wait()
    norm_second(0)
    widen(0)
    ar(AR_DENSE, 1, PASS)
    narrow_grad(0)
    ar(AR_DH2, 0, START)
    ar(AR_DENSE, 1, FINISH)
    norm_second(1)
    put(h2, o_h2)
    ar(AR_DH2, 0, MIDDLE)
    widen(1)
    put(gelu, o_gelu)
    put(dpre, o_dpre)
    narrow_grad(1)
    ar(AR_DH2, 1, START)
    narrow(0, 3)
    ar(AR_DH2, 1, MIDDLE)
    ar(AR_DH2, 0, PASS)
    narrow(3, 8)
    y_near.start()
    y_far.start()
    ar(AR_DH2, 0, FINISH)
    norm_second_grad(0)
    y_middle()
    attend_grad(0)
    ar(AR_DH2, 1, PASS)
    ar(AR_DH2, 1, FINISH)
    norm_second_grad(1)
    put(dr1, o_dr1)
    attend_grad(1)
    finish_kv()
    put(dqkv, o_dqkv)
    qkv_grad(0)
    ar(AR_DH1, 0, START)
    qkv_grad(1)
    ar(AR_DH1, 0, MIDDLE)
    ar(AR_DH1, 1, START)
    y_finish()
    ar(AR_DH1, 1, MIDDLE)
    ar(AR_DH1, 0, PASS)
    ar(AR_DH1, 0, FINISH)
    norm_first_grad(0)
    ar(AR_DH1, 1, PASS)
    ar(AR_DH1, 1, FINISH)
    norm_first_grad(1)
    put(dx, o_dx)
    for slot in range(8):
        o_small[slot:slot + 1, :] = jnp.sum(acc[slot], axis=0, keepdims=True)
    for copy in sends:
        copy.wait_send()
    for copy in outs:
        copy.wait()


def run_step(slopes, rows, w_qkv, w_dense, w_fc1, w_fc2, d_out, vectors, b_qkv):
    seq, width = rows.shape
    ffn = w_fc1.shape[1]
    hidden = w_dense.shape[0]
    heads, head_dim = w_qkv.shape[2], w_qkv.shape[3]
    block = seq // 4
    (emb_gain, emb_bias, ln1_gain, ln1_bias, b_dense, ln2_gain, ln2_bias, b_fc1, b_fc2) = vectors
    shape = jax.ShapeDtypeStruct
    any_spec = pl.BlockSpec(memory_space=ANY)
    vmem_spec = pl.BlockSpec(memory_space=VMEM)
    raw_rows = 256
    pitch = raw_rows + 8
    out_shapes = ([shape((seq, n), BF16) for n in (width, width, hidden, ffn, ffn, 3 * hidden, width, width, width)]
                  + [shape((block, width), BF16), shape((8, width), F32), shape((1, ffn), F32),
                     shape((1, 3 * hidden), F32)])
    scratch = [VMEM((2, raw_rows, 3, heads, head_dim), BF16), VMEM((3 * heads * pitch, head_dim), F32),
               VMEM((width, 3 * hidden), BF16), VMEM((hidden, width), BF16), VMEM((width, ffn), BF16),
               VMEM((ffn, width), BF16),
               VMEM((4, seq, width), BF16), VMEM((4, seq // 2, width), BF16), VMEM((4, seq, width), BF16),
               VMEM((4, seq, width), BF16), VMEM((seq, width), BF16),
               VMEM((seq, width), BF16), VMEM((2, block, width), BF16), VMEM((block, width), BF16),
               VMEM((block, width), BF16),
               VMEM((seq, width), BF16), VMEM((seq, width), BF16), VMEM((seq, 3 * hidden), BF16),
               VMEM((seq, hidden), BF16), VMEM((seq, width), BF16), VMEM((seq, width), BF16),
               VMEM((seq, ffn), BF16), VMEM((seq, ffn), F32), VMEM((seq, ffn), BF16),
               VMEM((heads, seq, seq), F32), VMEM((seq, width), BF16), VMEM((2, seq, hidden), F32),
               VMEM((seq, 3 * hidden), BF16), VMEM((seq, width), BF16), VMEM((1, 3 * hidden), F32),
               VMEM((8, 8, width), F32),
               pltpu.SemaphoreType.DMA((N_COPIES,)), pltpu.SemaphoreType.DMA((N_COPIES,)),
               pltpu.SemaphoreType.DMA((8,)), pltpu.SemaphoreType.DMA((9,))]
    return pl.pallas_call(
        functools.partial(step_kernel, slopes),
        out_shape=out_shapes,
        in_specs=[any_spec] * 6 + [vmem_spec] * 10,
        out_specs=[any_spec] * 9 + [vmem_spec] * 4,
        scratch_shapes=scratch,
        compiler_params=pltpu.CompilerParams(collective_id=0, has_side_effects=True, vmem_limit_bytes=MAX_VMEM),
        name='block_step',
    )(rows, w_qkv, w_dense, w_fc1, w_fc2, d_out, emb_gain, emb_bias, ln1_gain, ln1_bias, b_qkv, b_dense,
      ln2_gain, ln2_bias, b_fc1, b_fc2)


def weight_grad_kernel(lhs, rhs, out):
    rows = out.shape[0]
    out[...] = dot_tn(lhs[...], rhs[...]).astype(BF16)


def weight_grad(lhs, rhs, tile, name):
    tokens, rows = lhs.shape
    cols = rhs.shape[1]
    return pl.pallas_call(
        weight_grad_kernel,
        out_shape=jax.ShapeDtypeStruct((rows, cols), BF16),
        grid=(rows // tile,),
        in_specs=[pl.BlockSpec((tokens, tile), lambda i: (0, i)), pl.BlockSpec((tokens, cols), lambda i: (0, 0))],
        out_specs=pl.BlockSpec((tile, cols), lambda i: (i, 0)),
        name=name,
    )(lhs, rhs)


def qkv_weight_kernel(lhs, rhs, out, tmp):
    tile, _, heads, head_dim = out.shape
    pitch = tmp.shape[0] // (3 * heads)
    grad = dot_tn(lhs[...], rhs[...])
    for index in range(3 * heads):
        tmp[index * pitch:index * pitch + tile, :] = grad[:, index * head_dim:(index + 1) * head_dim]

    @pl.loop(0, tile // 8)
    def _(i):
        for j in range(8):
            for c in range(3):
                d = i * 8 + j
                out[d, c] = tmp[pl.ds(c * heads * pitch + d, heads, stride=pitch), :].astype(BF16)


def qkv_weight_grad(lhs, rhs, heads, head_dim):
    tokens, rows = lhs.shape
    tile = 256
    return pl.pallas_call(
        qkv_weight_kernel,
        out_shape=jax.ShapeDtypeStruct((rows, 3, heads, head_dim), BF16),
        grid=(rows // tile,),
        in_specs=[pl.BlockSpec((tokens, tile), lambda i: (0, i)),
                  pl.BlockSpec((tokens, 3 * heads * head_dim), lambda i: (0, 0))],
        out_specs=pl.BlockSpec((tile, 3, heads, head_dim), lambda i: (i, 0, 0, 0)),
        scratch_shapes=[VMEM((3 * heads * (tile + 8), head_dim), F32)],
        name='grad_qkv',
    )(lhs, rhs)


def table_grad_kernel(ids, grads, out):
    tile, tokens = out.shape[0], ids.shape[1]
    vocab_rows = tile * pl.num_programs(0)
    first = lax.axis_index('tp') * vocab_rows + pl.program_id(0) * tile
    row_id = lax.broadcasted_iota(jnp.int32, (tile, tokens), 0) + first
    pick = jnp.where(row_id == ids[...], 1.0, 0.0).astype(BF16)
    out[...] = dot_nn(pick, grads[...])


def table_grad(token_ids, grads, vocab_rows):
    tokens, width = grads.shape
    tile = 256
    return pl.pallas_call(
        table_grad_kernel,
        out_shape=jax.ShapeDtypeStruct((vocab_rows, width), F32),
        grid=(vocab_rows // tile,),
        in_specs=[pl.BlockSpec((1, tokens), lambda i: (0, 0)), pl.BlockSpec((tokens, width), lambda i: (0, 0))],
        out_specs=pl.BlockSpec((tile, width), lambda i: (i, 0)),
        name='grad_table',
    )(token_ids, grads)


def split_kernel(small, bqkv, bfc1, y_in, *outs):
    for slot in range(8):
        outs[slot][...] = small[slot:slot + 1, :]
    heads, head_dim = outs[8].shape[1], outs[8].shape[2]
    for c in range(3):
        for h in range(heads):
            lo = (c * heads + h) * head_dim
            outs[8][c, h:h + 1, :] = bqkv[0:1, lo:lo + head_dim]
    outs[9][...] = bfc1[...]
    outs[10][...] = y_in[...]


def split_small(small, bqkv, bfc1, y_part, heads, head_dim):
    shape = jax.ShapeDtypeStruct
    width = small.shape[1]
    spec = pl.BlockSpec(memory_space=VMEM)
    return pl.pallas_call(
        split_kernel,
        out_shape=[shape((1, width), F32)] * 8 + [shape((3, heads, head_dim), F32), shape(bfc1.shape, F32),
                                                   shape(y_part.shape, BF16)],
        in_specs=[spec] * 4,
        out_specs=[spec] * 11,
        name='split_small',
    )(small, bqkv, bfc1, y_part)


def device_step(slopes, token_ids, embed_table, emb_gain, emb_bias, ln1_gain, ln1_bias,
                w_qkv, b_qkv, w_dense, b_dense, ln2_gain, ln2_bias,
                w_fc1, b_fc1, w_fc2, b_fc2, d_out):
    heads, head_dim = w_qkv.shape[1], w_qkv.shape[3]
    rows = gather_rows(token_ids, embed_table)
    vectors = [v.reshape(1, -1) for v in (emb_gain, emb_bias, ln1_gain, ln1_bias, b_dense, ln2_gain, ln2_bias,
                                          b_fc1, b_fc2)]
    (h1, h2, ctx, gelu, dpre, dqkv, dy, dr1, dx, y_part, small, bfc1, bqkv) = run_step(
        slopes, rows, jnp.transpose(w_qkv, (0, 2, 1, 3)), w_dense, w_fc1, w_fc2, d_out[0], vectors,
        jnp.transpose(b_qkv, (1, 0, 2)))
    d_w_qkv = jnp.transpose(qkv_weight_grad(h1, dqkv, heads, head_dim), (0, 2, 1, 3))
    d_w_dense = weight_grad(ctx, dr1, 256, 'grad_dense')
    d_w_fc1 = weight_grad(h2, dpre, 256, 'grad_fc1')
    d_w_fc2 = weight_grad(gelu, dy, 256, 'grad_fc2')
    d_table = table_grad(token_ids, dx, embed_table.shape[0])
    outs = split_small(small, bqkv, bfc1, y_part, heads, head_dim)
    vec = [v.reshape(-1) for v in outs[:8]]
    d_b_qkv = jnp.transpose(outs[8], (1, 0, 2))
    return (outs[10][None], d_table, vec[ACC_EG], vec[ACC_EB], vec[ACC_L1G], vec[ACC_L1B],
            d_w_qkv, d_b_qkv, d_w_dense, vec[ACC_BD], vec[ACC_L2G], vec[ACC_L2B],
            d_w_fc1, outs[9].reshape(-1), d_w_fc2, vec[ACC_BF2])


def solution(mesh):
    in_specs = (P('dp', None), P('tp', None), P(None), P(None), P(None), P(None),
                P(None, 'tp', None, None), P('tp', None, None), P('tp', None), P(None),
                P(None), P(None), P(None, 'tp'), P('tp'), P('tp', None), P(None),
                P('dp', 'tp', None))
    out_specs = (P('dp', 'tp', None), P(('dp', 'tp'), None), P('dp'), P('dp'), P('dp'), P('dp'),
                 P('dp', 'tp', None, None), P(('dp', 'tp'), None, None), P(('dp', 'tp'), None), P('dp'),
                 P('dp'), P('dp'), P('dp', 'tp'), P(('dp', 'tp')), P(('dp', 'tp'), None), P('dp'))

    def run(*arrays):
        slopes = alibi_slopes(arrays[6].shape[1])
        step = functools.partial(device_step, slopes)
        mapped = jax.shard_map(step, mesh=mesh, in_specs=in_specs, out_specs=out_specs, check_vma=False)
        return mapped(*arrays)

    return run
```

```python
import functools
import jax
import jax.numpy as jnp
from jax import lax
from jax.experimental import pallas as pl
from jax.experimental.pallas import tpu as pltpu
from jax.sharding import PartitionSpec as P

EPS = 1e-5
F32 = jnp.float32
BF16 = jnp.bfloat16
VMEM = pltpu.VMEM
ANY = pl.ANY
MAX_VMEM = 67_043_328
NT_DIMS = (((1,), (1,)), ((), ()))
TN_DIMS = (((0,), (0,)), ((), ()))
GELU_A = 0.7978845608028654
GELU_B = 0.044715


def alibi_slopes(head_count):
    closest = 2 ** (head_count.bit_length() - 1)
    slope_base = 2.0 ** (-8.0 / closest)
    extra_base = 2.0 ** (-4.0 / closest)
    slopes = [slope_base ** exponent for exponent in range(1, closest + 1)]
    return slopes + [extra_base ** exponent for exponent in range(1, 2 * (head_count - closest), 2)]


def dot_nn(lhs, rhs):
    return jnp.dot(lhs, rhs, preferred_element_type=F32)


def dot_nt(lhs, rhs):
    return lax.dot_general(lhs, rhs, NT_DIMS, preferred_element_type=F32)


def dot_tn(lhs, rhs):
    return lax.dot_general(lhs, rhs, TN_DIMS, preferred_element_type=F32)


def normalize(values):
    centered = values - jnp.mean(values, axis=-1, keepdims=True)
    inv_std = lax.rsqrt(jnp.mean(centered * centered, axis=-1, keepdims=True) + EPS)
    return centered * inv_std, inv_std


def norm_backward(d_norm, x_hat, inv_std, gain_vec):
    d_hat = d_norm * gain_vec
    return inv_std * (d_hat - jnp.mean(d_hat, axis=-1, keepdims=True)
                      - x_hat * jnp.mean(d_hat * x_hat, axis=-1, keepdims=True))


def gather_kernel(ids_smem, ids_vmem, table, out, stage, rows_buf, load_sem, out_sem):
    tokens = ids_smem.shape[1]
    vocab_rows = table.shape[0]
    base = lax.axis_index('tp') * vocab_rows
    groups, group = load_sem.shape[0], tokens // load_sem.shape[0]
    span = group * 8

    @pl.loop(0, groups)
    def _(block):
        @pl.loop(0, group, unroll=8)
        def _(i):
            token = block * group + i
            row = lax.rem(ids_smem[0, token], vocab_rows)
            first = pl.multiple_of((row >> 3) << 3, 8)
            pltpu.make_async_copy(table.at[pl.ds(first, 8), :],
                                  stage.at[pl.ds(pl.multiple_of(token * 8, 8), 8), :], load_sem.at[block]).start()

    local = ids_vmem[...] - base
    inside = jnp.where(local >= 0, 1, 0) * jnp.where(local < vocab_rows, 1, 0)
    sub = jnp.where(inside > 0, local & 7, -span)
    index = lax.broadcasted_iota(jnp.int32, (span, group), 0)
    lane = lax.broadcasted_iota(jnp.int32, (span, group), 1) * 8
    copies = []
    for block in range(groups):
        pick = jnp.where(index == lane + sub[:, block * group:(block + 1) * group], 1.0, 0.0).astype(BF16)
        part = slice(block * span, (block + 1) * span)
        rows = slice(block * group, (block + 1) * group)
        pltpu.make_async_copy(table.at[pl.ds(0, span), :], stage.at[part, :], load_sem.at[block]).wait()
        rows_buf[rows, :] = dot_tn(pick, stage[part, :]).astype(BF16)
        copies.append(pltpu.make_async_copy(rows_buf.at[rows, :], out.at[rows, :], out_sem.at[block]))
        copies[-1].start()
    for copy in copies:
        copy.wait()


def gather_rows(token_ids, table):
    tokens, width = token_ids.shape[1], table.shape[1]
    groups = 8
    return pl.pallas_call(
        gather_kernel,
        out_shape=jax.ShapeDtypeStruct((tokens, width), BF16),
        in_specs=[pl.BlockSpec(memory_space=pltpu.SMEM), pl.BlockSpec(memory_space=VMEM),
                  pl.BlockSpec(memory_space=ANY)],
        out_specs=pl.BlockSpec(memory_space=ANY),
        scratch_shapes=[VMEM((tokens * 8, width), BF16), VMEM((tokens, width), BF16),
                        pltpu.SemaphoreType.DMA((groups,)), pltpu.SemaphoreType.DMA((groups,))],
        compiler_params=pltpu.CompilerParams(vmem_limit_bytes=MAX_VMEM),
        name='gather_rows',
    )(token_ids, token_ids, table)


CHUNKS = 2
ROW_STEP = 64
WIDEN_TILE = 1024
ROW_UNROLL = 1
AR_EMB, AR_DENSE, AR_DH2, AR_DH1 = range(4)
(ACC_EG, ACC_EB, ACC_L1G, ACC_L1B, ACC_BD, ACC_L2G, ACC_L2B, ACC_BF2) = range(8)
N_COPIES = 4 * CHUNKS * 4 + 3 + 3


def step_kernel(slopes, rows_in, w_qkv, w_dense, w_fc1, w_fc2, d_out,
                emb_gain, emb_bias, ln1_gain, ln1_bias, b_qkv, b_dense, ln2_gain, ln2_bias, b_fc1, b_fc2,
                o_h1, o_h2, o_ctx, o_gelu, o_dpre, o_dqkv, o_dy, o_dr1, o_dx, y_out, o_small, o_bfc1, o_bqkv,
                wraw, wtmp, wq, wd, w1, w2, part, din, summ, cross, dy, ypart, y_in, y_send, y_cross,
                emb, h1, qkv, ctx, r1, h2, gelu, dgelu, dpre, prob, dr1, d_kv, dqkv, dx, bq, acc,
                send_sem, recv_sem, load_sem, out_sem):
    tp = lax.axis_index('tp')
    core = lax.rem(tp, 2)
    chip = tp // 2
    partner = tp + 1 - 2 * core
    xpeer = lax.rem(tp + 2, 4)
    seq, width = emb.shape
    size = seq // CHUNKS
    half = size // 2
    heads, head_dim = b_qkv.shape[1], b_qkv.shape[2]
    scale = head_dim ** -0.5
    hidden = heads * head_dim
    block = seq // 4

    barrier = pltpu.get_barrier_semaphore()
    for peer in (partner, xpeer):
        pl.semaphore_signal(barrier, inc=1, device_id={'tp': peer}, device_id_type=pl.DeviceIdType.MESH)

    def load(src, dst, index):
        copy = pltpu.make_async_copy(src, dst, load_sem.at[index])
        copy.start()
        return copy

    load_rows = load(rows_in, part.at[AR_EMB], 0)
    my_block = pl.ds(pl.multiple_of(tp * block, block), block)
    load_dy = load(d_out, dy.at[my_block, :], 1)
    raw_rows = wraw.shape[1]
    raw_steps = w_qkv.shape[0] // raw_rows

    def load_raw(step):
        return pltpu.make_async_copy(w_qkv.at[pl.ds(pl.multiple_of(step * raw_rows, raw_rows), raw_rows)],
                                     wraw.at[lax.rem(step, 2)], load_sem.at[6 + lax.rem(step, 2)])

    load_raw(0).start()
    load_raw(1).start()
    load_wd = load(w_dense, wd, 2)
    load_w2 = load(w_fc2, w2, 3)
    load_w1 = load(w_fc1, w1, 4)

    count = [0]
    sends = []

    def remote(src, dst, peer):
        index = count[0]
        count[0] += 1
        copy = pltpu.make_async_remote_copy(src_ref=src, dst_ref=dst, send_sem=send_sem.at[index],
                                            recv_sem=recv_sem.at[index], device_id={'tp': peer},
                                            device_id_type=pl.DeviceIdType.MESH)
        sends.append(copy)
        return copy

    def at_row(start, length):
        return pl.ds(pl.multiple_of(start, half), length)

    def make_reduce(which, chunk):
        base = chunk * size
        mine, other = at_row(base + core * half, half), at_row(base + (1 - core) * half, half)
        local_in = din.at[which, pl.ds(chunk * half, half), :]
        first = remote(part.at[which, other, :], local_in, partner)
        across = remote(summ.at[which, mine, :], cross.at[which, mine, :], xpeer)
        share = remote(summ.at[which, mine, :], summ.at[which, mine, :], partner)
        forward = remote(cross.at[which, mine, :], cross.at[which, mine, :], partner)

        def middle():
            first.wait_recv()

            @pl.loop(0, half // 16)
            def _(i):
                rows = pl.ds(pl.multiple_of(base + core * half + i * 16, 16), 16)
                got = din[which, pl.ds(pl.multiple_of(chunk * half + i * 16, 16), 16), :]
                summ[which, rows, :] = (part[which, rows, :].astype(F32) + got.astype(F32)).astype(BF16)

            across.start()
            share.start()

        def pass_on():
            across.wait_recv()
            forward.start()

        def finish():
            share.wait_recv()
            forward.wait_recv()

        return first.start, middle, pass_on, finish

    reduces = {(w, c): make_reduce(w, c) for w in range(4) for c in range(CHUNKS)}

    def ar(which, chunk, stage):
        reduces[which, chunk][stage]()

    dy_across = remote(dy.at[my_block, :], dy.at[my_block, :], xpeer)
    dy_share = remote(dy.at[my_block, :], dy.at[my_block, :], partner)
    peer_block = pl.ds(pl.multiple_of(xpeer * block, block), block)
    dy_forward = remote(dy.at[peer_block, :], dy.at[peer_block, :], partner)

    partner_block = pl.ds(pl.multiple_of(partner * block, block), block)
    far = 2 * (1 - chip) + 1 - core
    far_block = pl.ds(pl.multiple_of(far * block, block), block)
    y_near = remote(ypart.at[partner_block, :], y_in.at[0], partner)
    y_far = remote(ypart.at[far_block, :], y_in.at[1], partner)
    y_over = remote(y_send, y_cross, xpeer)

    outs = []

    def put(src, dst):
        copy = pltpu.make_async_copy(src, dst, out_sem.at[len(outs)])
        copy.start()
        outs.append(copy)

    def row_loop(chunk, body, step=ROW_STEP):
        @pl.loop(0, size // step, unroll=ROW_UNROLL)
        def _(i):
            body(pl.ds(pl.multiple_of(chunk * size + i * step, step), step))

    def chunk_rows(chunk):
        return slice(chunk * size, (chunk + 1) * size)

    def col_loop(total, tile, body, first=0):
        @pl.loop(first, total // tile)
        def _(n):
            body(pl.ds(pl.multiple_of(n * tile, tile), tile))

    def accumulate(slot, values):
        total = values[:8]
        for first in range(8, values.shape[0], 8):
            total = total + values[first:first + 8]
        acc[slot] += total

    def exchanged(which, rows):
        return summ[which, rows, :].astype(F32) + cross[which, rows, :].astype(F32)

    def unpack_qkv():
        pitch = wtmp.shape[0] // (3 * heads)
        for c in range(3):
            for h in range(heads):
                bq[0:1, c * hidden + h * head_dim:c * hidden + (h + 1) * head_dim] = b_qkv[c, h:h + 1, :]

        @pl.loop(0, raw_steps)
        def _(step):
            load_raw(step).wait()
            slot = lax.rem(step, 2)

            @pl.loop(0, raw_rows // 8)
            def _(i):
                for j in range(8):
                    for c in range(3):
                        d = i * 8 + j
                        wtmp[pl.ds(c * heads * pitch + d, heads, stride=pitch), :] = wraw[slot, d, c].astype(F32)

            @pl.when(step + 2 < raw_steps)
            def _():
                load_raw(step + 2).start()

            dst = pl.ds(pl.multiple_of(step * raw_rows, raw_rows), raw_rows)
            for c in range(3):
                for h in range(heads):
                    lo = c * hidden + h * head_dim
                    wq[dst, lo:lo + head_dim] = wtmp[(c * heads + h) * pitch:
                                                     (c * heads + h) * pitch + raw_rows, :].astype(BF16)

    def norm_first(chunk):
        def body(rows):
            x_hat, _ = normalize(exchanged(AR_EMB, rows))
            embedded = (x_hat * emb_gain[...] + emb_bias[...]).astype(BF16)
            emb[rows, :] = embedded
            e_hat, _ = normalize(embedded.astype(F32))
            h1[rows, :] = (e_hat * ln1_gain[...] + ln1_bias[...]).astype(BF16)

        row_loop(chunk, body)

    def project_qkv(chunk):
        rows = chunk_rows(chunk)

        def body(cols):
            qkv[rows, cols] = (dot_nn(h1[rows, :], wq[:, cols]) + bq[0:1, cols]).astype(BF16)

        col_loop(3 * hidden, 768, body)

    def head_cols(part_index, h):
        lo = part_index * hidden + h * head_dim
        return slice(lo, lo + head_dim)

    def attend(chunk):
        rows = chunk_rows(chunk)
        keys = (chunk + 1) * size
        row_id = lax.broadcasted_iota(jnp.int32, (size, keys), 0) + chunk * size
        col_id = lax.broadcasted_iota(jnp.int32, (size, keys), 1)
        rel = (col_id - row_id).astype(F32)
        for h in range(heads):
            slope = F32(slopes[3 * heads + h])
            for t in (2, 1, 0):
                slope = jnp.where(tp == t, F32(slopes[t * heads + h]), slope)
            scores = dot_nt(qkv[rows, head_cols(0, h)], qkv[0:keys, head_cols(1, h)]) * scale
            scores = jnp.where(col_id <= row_id, scores + slope * rel, -1e30)
            top = jnp.max(scores, axis=-1, keepdims=True)
            weight = jnp.exp(scores - top)
            p = weight / jnp.sum(weight, axis=-1, keepdims=True)
            prob[h, rows, 0:keys] = p
            ctx[rows, h * head_dim:(h + 1) * head_dim] = dot_nn(
                p.astype(BF16), qkv[0:keys, head_cols(2, h)]).astype(BF16)

    def project_dense(chunk):
        rows = chunk_rows(chunk)

        def body(cols):
            part[AR_DENSE, rows, cols] = dot_nn(ctx[rows, :], wd[:, cols]).astype(BF16)

        col_loop(width, 1024, body)

    def norm_second(chunk):
        def body(rows):
            r_one = (emb[rows, :].astype(F32) + exchanged(AR_DENSE, rows) + b_dense[...]).astype(BF16)
            r1[rows, :] = r_one
            r_hat, _ = normalize(r_one.astype(F32))
            h2[rows, :] = (r_hat * ln2_gain[...] + ln2_bias[...]).astype(BF16)

        row_loop(chunk, body)

    def gelu_grad(first, last):
        @pl.loop(first, last)
        def _(n):
            cols = pl.ds(pl.multiple_of(n * 512, 512), 512)
            dgelu[:, cols] = dot_nt(dy[...], w2[cols, :])

    def widen(chunk):
        rows = chunk_rows(chunk)

        def body(cols):
            pre = dot_nn(h2[rows, :], w1[:, cols]) + b_fc1[0:1, cols]
            square = pre * pre
            bend = jnp.tanh(GELU_A * (pre + GELU_B * (pre * square)))
            gelu[rows, cols] = (0.5 * pre * (1.0 + bend)).astype(BF16)
            slope = 0.5 * (1.0 + bend) + 0.5 * pre * (1.0 - bend * bend) * (GELU_A * (1.0 + 3.0 * GELU_B * square))
            d_pre = dgelu[rows, cols] * slope
            dpre[rows, cols] = d_pre.astype(BF16)
            total = jnp.sum(d_pre, axis=0, keepdims=True)
            o_bfc1[0:1, cols] = total if chunk == 0 else o_bfc1[0:1, cols] + total

        col_loop(w1.shape[1], WIDEN_TILE, body)

    def narrow_grad(chunk):
        rows = chunk_rows(chunk)

        def body(cols):
            part[AR_DH2, rows, cols] = dot_nt(dpre[rows, :], w1[cols, :]).astype(BF16)

        col_loop(width, 1024, body)

    def narrow(first, last):
        @pl.loop(first, last)
        def _(n):
            cols = pl.ds(pl.multiple_of(n * 512, 512), 512)
            ypart[:, cols] = dot_nn(gelu[...], w2[:, cols]).astype(BF16)

    def y_middle():
        y_near.wait_recv()
        y_far.wait_recv()

        @pl.loop(0, block // 16)
        def _(i):
            rows = pl.ds(pl.multiple_of(i * 16, 16), 16)
            src = pl.ds(pl.multiple_of(xpeer * block + i * 16, 16), 16)
            y_send[rows, :] = (ypart[src, :].astype(F32) + y_in[1, rows, :].astype(F32)).astype(BF16)

        y_over.start()

    def y_finish():
        y_over.wait_recv()

        @pl.loop(0, block // 16)
        def _(i):
            rows = pl.ds(pl.multiple_of(i * 16, 16), 16)
            src = pl.ds(pl.multiple_of(tp * block + i * 16, 16), 16)
            total = ypart[src, :].astype(F32) + y_in[0, rows, :].astype(F32) + y_cross[rows, :].astype(F32)
            y_out[rows, :] = (r1[src, :].astype(F32) + total + b_fc2[...]).astype(BF16)

    def norm_second_grad(chunk):
        def body(rows):
            r_hat, inv = normalize(r1[rows, :].astype(F32))
            d_norm = exchanged(AR_DH2, rows)
            dy_rows = dy[rows, :].astype(F32)
            grad = dy_rows + norm_backward(d_norm, r_hat, inv, ln2_gain[...])
            dr1[rows, :] = grad.astype(BF16)
            accumulate(ACC_L2G, d_norm * r_hat)
            accumulate(ACC_L2B, d_norm)
            accumulate(ACC_BD, grad)
            accumulate(ACC_BF2, dy_rows)

        row_loop(chunk, body)

    def attend_grad(chunk):
        rows = chunk_rows(chunk)
        keys = (chunk + 1) * size
        old = chunk * size
        for h in range(heads):
            cols = slice(h * head_dim, (h + 1) * head_dim)
            d_ctx = dot_nt(dr1[rows, :], wd[cols, :]).astype(BF16)
            p = prob[h, rows, 0:keys]
            d_prob = dot_nt(d_ctx, qkv[0:keys, head_cols(2, h)])
            d_score = p * (d_prob - jnp.sum(d_prob * p, axis=-1, keepdims=True))
            d_score = (d_score * scale).astype(BF16)
            d_query = dot_nn(d_score, qkv[0:keys, head_cols(1, h)])
            dqkv[rows, head_cols(0, h)] = d_query.astype(BF16)
            total = jnp.sum(d_query, axis=0, keepdims=True)
            o_bqkv[0:1, head_cols(0, h)] = total if chunk == 0 else o_bqkv[0:1, head_cols(0, h)] + total
            for index, grad in ((0, dot_tn(d_score, qkv[rows, head_cols(0, h)])),
                                (1, dot_tn(p.astype(BF16), d_ctx))):
                if old:
                    d_kv[index, 0:old, cols] += grad[:old]
                d_kv[index, old:keys, cols] = grad[old:]

    def finish_kv():
        for index in range(2):
            lo = (index + 1) * hidden
            dqkv[:, lo:lo + hidden] = d_kv[index].astype(BF16)
            o_bqkv[0:1, lo:lo + hidden] = jnp.sum(d_kv[index], axis=0, keepdims=True)

    def qkv_grad(chunk):
        rows = chunk_rows(chunk)

        def body(cols):
            part[AR_DH1, rows, cols] = dot_nt(dqkv[rows, :], wq[cols, :]).astype(BF16)

        col_loop(width, 1024, body)

    def norm_first_grad(chunk):
        def body(rows):
            e_hat, e_inv = normalize(emb[rows, :].astype(F32))
            d_norm = exchanged(AR_DH1, rows)
            grad = dr1[rows, :].astype(F32) + norm_backward(d_norm, e_hat, e_inv, ln1_gain[...])
            accumulate(ACC_L1G, d_norm * e_hat)
            accumulate(ACC_L1B, d_norm)
            x_hat, x_inv = normalize(exchanged(AR_EMB, rows))
            accumulate(ACC_EG, grad * x_hat)
            accumulate(ACC_EB, grad)
            dx[rows, :] = norm_backward(grad, x_hat, x_inv, emb_gain[...]).astype(BF16)

        row_loop(chunk, body)

    START, MIDDLE, PASS, FINISH = range(4)
    acc[...] = jnp.zeros_like(acc)
    load_rows.wait()
    pl.semaphore_wait(barrier, 2)
    ar(AR_EMB, 0, START)
    ar(AR_EMB, 1, START)
    ar(AR_EMB, 0, MIDDLE)
    ar(AR_EMB, 1, MIDDLE)
    load_dy.wait()
    dy_across.start()
    dy_share.start()
    unpack_qkv()
    load_wd.wait()
    ar(AR_EMB, 0, PASS)
    ar(AR_EMB, 0, FINISH)
    norm_first(0)
    project_qkv(0)
    ar(AR_EMB, 1, PASS)
    attend(0)
    project_dense(0)
    ar(AR_DENSE, 0, START)
    ar(AR_EMB, 1, FINISH)
    norm_first(1)
    put(h1, o_h1)
    ar(AR_DENSE, 0, MIDDLE)
    project_qkv(1)
    dy_across.wait_recv()
    dy_forward.start()
    attend(1)
    put(ctx, o_ctx)
    project_dense(1)
    ar(AR_DENSE, 1, START)
    dy_share.wait_recv()
    dy_forward.wait_recv()
    put(dy, o_dy)
    load_w2.wait()
    gelu_grad(0, 1)
    ar(AR_DENSE, 1, MIDDLE)
    gelu_grad(1, 4)
    ar(AR_DENSE, 0, PASS)
    ar(AR_DENSE, 0, FINISH)
    load_w1.wait()
    norm_second(0)
    widen(0)
    ar(AR_DENSE, 1, PASS)
    narrow_grad(0)
    ar(AR_DH2, 0, START)
    ar(AR_DENSE, 1, FINISH)
    norm_second(1)
    put(h2, o_h2)
    ar(AR_DH2, 0, MIDDLE)
    widen(1)
    put(gelu, o_gelu)
    put(dpre, o_dpre)
    narrow_grad(1)
    ar(AR_DH2, 1, START)
    narrow(0, 2)
    ar(AR_DH2, 1, MIDDLE)
    ar(AR_DH2, 0, PASS)
    narrow(2, 4)
    y_near.start()
    y_far.start()
    ar(AR_DH2, 0, FINISH)
    norm_second_grad(0)
    y_middle()
    attend_grad(0)
    ar(AR_DH2, 1, PASS)
    ar(AR_DH2, 1, FINISH)
    norm_second_grad(1)
    put(dr1, o_dr1)
    attend_grad(1)
    finish_kv()
    put(dqkv, o_dqkv)
    qkv_grad(0)
    ar(AR_DH1, 0, START)
    qkv_grad(1)
    ar(AR_DH1, 0, MIDDLE)
    ar(AR_DH1, 1, START)
    y_finish()
    ar(AR_DH1, 1, MIDDLE)
    ar(AR_DH1, 0, PASS)
    ar(AR_DH1, 0, FINISH)
    norm_first_grad(0)
    ar(AR_DH1, 1, PASS)
    ar(AR_DH1, 1, FINISH)
    norm_first_grad(1)
    put(dx, o_dx)
    for slot in range(8):
        o_small[slot:slot + 1, :] = jnp.sum(acc[slot], axis=0, keepdims=True)
    for copy in sends:
        copy.wait_send()
    for copy in outs:
        copy.wait()


def run_step(slopes, rows, w_qkv, w_dense, w_fc1, w_fc2, d_out, vectors, b_qkv):
    seq, width = rows.shape
    ffn = w_fc1.shape[1]
    hidden = w_dense.shape[0]
    heads, head_dim = w_qkv.shape[2], w_qkv.shape[3]
    block = seq // 4
    (emb_gain, emb_bias, ln1_gain, ln1_bias, b_dense, ln2_gain, ln2_bias, b_fc1, b_fc2) = vectors
    shape = jax.ShapeDtypeStruct
    any_spec = pl.BlockSpec(memory_space=ANY)
    vmem_spec = pl.BlockSpec(memory_space=VMEM)
    raw_rows = 256
    pitch = raw_rows + 8
    out_shapes = ([shape((seq, n), BF16) for n in (width, width, hidden, ffn, ffn, 3 * hidden, width, width, width)]
                  + [shape((block, width), BF16), shape((8, width), F32), shape((1, ffn), F32),
                     shape((1, 3 * hidden), F32)])
    scratch = [VMEM((2, raw_rows, 3, heads, head_dim), BF16), VMEM((3 * heads * pitch, head_dim), F32),
               VMEM((width, 3 * hidden), BF16), VMEM((hidden, width), BF16), VMEM((width, ffn), BF16),
               VMEM((ffn, width), BF16),
               VMEM((4, seq, width), BF16), VMEM((4, seq // 2, width), BF16), VMEM((4, seq, width), BF16),
               VMEM((4, seq, width), BF16), VMEM((seq, width), BF16),
               VMEM((seq, width), BF16), VMEM((2, block, width), BF16), VMEM((block, width), BF16),
               VMEM((block, width), BF16),
               VMEM((seq, width), BF16), VMEM((seq, width), BF16), VMEM((seq, 3 * hidden), BF16),
               VMEM((seq, hidden), BF16), VMEM((seq, width), BF16), VMEM((seq, width), BF16),
               VMEM((seq, ffn), BF16), VMEM((seq, ffn), F32), VMEM((seq, ffn), BF16),
               VMEM((heads, seq, seq), F32), VMEM((seq, width), BF16), VMEM((2, seq, hidden), F32),
               VMEM((seq, 3 * hidden), BF16), VMEM((seq, width), BF16), VMEM((1, 3 * hidden), F32),
               VMEM((8, 8, width), F32),
               pltpu.SemaphoreType.DMA((N_COPIES,)), pltpu.SemaphoreType.DMA((N_COPIES,)),
               pltpu.SemaphoreType.DMA((8,)), pltpu.SemaphoreType.DMA((9,))]
    return pl.pallas_call(
        functools.partial(step_kernel, slopes),
        out_shape=out_shapes,
        in_specs=[any_spec] * 6 + [vmem_spec] * 10,
        out_specs=[any_spec] * 9 + [vmem_spec] * 4,
        scratch_shapes=scratch,
        compiler_params=pltpu.CompilerParams(collective_id=0, has_side_effects=True, vmem_limit_bytes=MAX_VMEM),
        name='block_step',
    )(rows, w_qkv, w_dense, w_fc1, w_fc2, d_out, emb_gain, emb_bias, ln1_gain, ln1_bias, b_qkv, b_dense,
      ln2_gain, ln2_bias, b_fc1, b_fc2)


TABLE_TILE = 1024
WEIGHT_TILE = 1024
QKV_TILE = 256


def grads_kernel(ids, small, bqkv, bfc1, y_part, h1_in, h2_in, ctx_in, gelu_in, dpre_in, dqkv_in, dy_in, dr1_in, dx_in,
                 *refs):
    vec_out, (o_bqkv, o_bfc1, o_y, o_table, o_qkv, o_dense, o_fc1, o_fc2) = refs[:8], refs[8:16]
    (h1, h2, ctx, gelu, dpre, dqkv, dy, dr1, dx, table_ring, weight_ring, qkv_ring, tmp,
     load_sem, table_sem, weight_sem, qkv_sem, y_sem) = refs[16:]
    _, heads, head_dim = o_bqkv.shape
    tokens, width = dx.shape
    vocab_rows = o_table.shape[0]
    loads = {}
    for index, (src, dst) in enumerate(((dx_in, dx), (h1_in, h1), (dqkv_in, dqkv), (h2_in, h2), (dpre_in, dpre),
                                        (gelu_in, gelu), (dy_in, dy), (ctx_in, ctx), (dr1_in, dr1))):
        loads[index] = pltpu.make_async_copy(src, dst, load_sem.at[index])
        loads[index].start()
    copy_y = pltpu.make_async_copy(y_part, o_y, y_sem)
    copy_y.start()
    for slot in range(8):
        vec_out[slot][...] = small[slot:slot + 1, :]
    for c in range(3):
        for h in range(heads):
            lo = (c * heads + h) * head_dim
            o_bqkv[c, h:h + 1, :] = bqkv[0:1, lo:lo + head_dim]
    o_bfc1[...] = bfc1[...]

    first_row = lax.axis_index('tp') * vocab_rows
    pitch = tmp.shape[0] // (3 * heads)

    def table_copy(step):
        slot = lax.rem(step, 2)
        return pltpu.make_async_copy(
            table_ring.at[slot], o_table.at[pl.ds(pl.multiple_of(step * TABLE_TILE, TABLE_TILE), TABLE_TILE), :],
            table_sem.at[slot])

    def qkv_copy(step, slot):
        return pltpu.make_async_copy(
            qkv_ring.at[slot], o_qkv.at[pl.ds(pl.multiple_of(step * QKV_TILE, QKV_TILE), QKV_TILE)],
            qkv_sem.at[slot])

    def qkv_step(step, slot):
        cols = pl.ds(pl.multiple_of(step * QKV_TILE, QKV_TILE), QKV_TILE)
        grad = dot_tn(h1[:, cols], dqkv[...])
        for index in range(3 * heads):
            tmp[index * pitch:index * pitch + QKV_TILE, :] = grad[:, index * head_dim:(index + 1) * head_dim]

        @pl.loop(0, QKV_TILE // 32)
        def _(i):
            for j in range(32):
                for c in range(3):
                    d = i * 32 + j
                    qkv_ring[slot, d, c] = tmp[pl.ds(c * heads * pitch + d, heads, stride=pitch), :].astype(BF16)

        qkv_copy(step, slot).start()

    table_steps = vocab_rows // TABLE_TILE
    qkv_per = width // QKV_TILE // table_steps
    loads[0].wait()

    @pl.loop(0, table_steps)
    def _(step):
        slot = lax.rem(step, 2)

        @pl.when(step >= 2)
        def _():
            table_copy(step - 2).wait()

        row_id = lax.broadcasted_iota(jnp.int32, (TABLE_TILE, tokens), 0) + (first_row + step * TABLE_TILE)
        pick = jnp.where(row_id == ids[...], 1.0, 0.0).astype(BF16)
        table_ring[slot] = dot_nn(pick, dx[...])
        table_copy(step).start()

        @pl.when(step == 0)
        def _():
            loads[1].wait()
            loads[2].wait()

        for sub in range(qkv_per):
            @pl.when(step >= 1)
            def _():
                qkv_copy((step - 1) * qkv_per + sub, sub).wait()

            qkv_step(step * qkv_per + sub, sub)

    pending = {}
    order = []
    for lhs, rhs, out, needs in ((h2, dpre, o_fc1, (3, 4)), (gelu, dy, o_fc2, (5, 6)), (ctx, dr1, o_dense, (7, 8))):
        tile = min(WEIGHT_TILE, lhs.shape[1])
        for step in range(lhs.shape[1] // tile):
            order.append((lhs, rhs, out, needs if step == 0 else (), step * tile, tile))
    for index, (lhs, rhs, out, needs, lo, tile) in enumerate(order):
        slot = index % 2
        for load in needs:
            loads[load].wait()
        if slot in pending:
            pending[slot].wait()
        weight_ring[slot, 0:tile, :] = dot_tn(lhs[:, lo:lo + tile], rhs[...]).astype(BF16)
        pending[slot] = pltpu.make_async_copy(weight_ring.at[slot, 0:tile, :], out.at[lo:lo + tile, :],
                                              weight_sem.at[slot])
        pending[slot].start()

    for step in range(table_steps - 2, table_steps):
        table_copy(step).wait()
    for sub in range(qkv_per):
        qkv_copy((table_steps - 1) * qkv_per + sub, sub).wait()
    for copy in pending.values():
        copy.wait()
    copy_y.wait()


def all_grads(token_ids, vocab_rows, heads, head_dim, small, bqkv, bfc1, y_part, acts):
    shape = jax.ShapeDtypeStruct
    tokens, width = acts[0].shape
    ffn, hidden = acts[3].shape[1], heads * head_dim
    vmem_spec, any_spec = pl.BlockSpec(memory_space=VMEM), pl.BlockSpec(memory_space=ANY)
    table_steps = vocab_rows // TABLE_TILE
    qkv_per = width // QKV_TILE // table_steps
    return pl.pallas_call(
        grads_kernel,
        out_shape=[shape((1, width), F32)] * 8 + [
            shape((3, heads, head_dim), F32), shape(bfc1.shape, F32), shape(y_part.shape, BF16),
            shape((vocab_rows, width), F32), shape((width, 3, heads, head_dim), BF16), shape((hidden, width), BF16),
            shape((width, ffn), BF16), shape((ffn, width), BF16)],
        in_specs=[vmem_spec] * 4 + [any_spec] * 10,
        out_specs=[vmem_spec] * 10 + [any_spec] * 6,
        scratch_shapes=[VMEM(a.shape, BF16) for a in acts] + [
            VMEM((2, TABLE_TILE, width), F32), VMEM((2, WEIGHT_TILE, width), BF16),
            VMEM((qkv_per, QKV_TILE, 3, heads, head_dim), BF16), VMEM((3 * heads * (QKV_TILE + 8), head_dim), F32),
            pltpu.SemaphoreType.DMA((len(acts),)), pltpu.SemaphoreType.DMA((2,)), pltpu.SemaphoreType.DMA((2,)),
            pltpu.SemaphoreType.DMA((qkv_per,)), pltpu.SemaphoreType.DMA],
        compiler_params=pltpu.CompilerParams(vmem_limit_bytes=MAX_VMEM),
        name='all_grads',
    )(token_ids, small, bqkv, bfc1, y_part, *acts)


def device_step(slopes, token_ids, embed_table, emb_gain, emb_bias, ln1_gain, ln1_bias,
                w_qkv, b_qkv, w_dense, b_dense, ln2_gain, ln2_bias,
                w_fc1, b_fc1, w_fc2, b_fc2, d_out):
    heads, head_dim = w_qkv.shape[1], w_qkv.shape[3]
    rows = gather_rows(token_ids, embed_table)
    vectors = [v.reshape(1, -1) for v in (emb_gain, emb_bias, ln1_gain, ln1_bias, b_dense, ln2_gain, ln2_bias,
                                          b_fc1, b_fc2)]
    (h1, h2, ctx, gelu, dpre, dqkv, dy, dr1, dx, y_part, small, bfc1, bqkv) = run_step(
        slopes, rows, jnp.transpose(w_qkv, (0, 2, 1, 3)), w_dense, w_fc1, w_fc2, d_out[0], vectors,
        jnp.transpose(b_qkv, (1, 0, 2)))
    outs = all_grads(token_ids, embed_table.shape[0], heads, head_dim, small, bqkv, bfc1, y_part,
                     (h1, h2, ctx, gelu, dpre, dqkv, dy, dr1, dx))
    d_table, d_w_dense, d_w_fc1, d_w_fc2 = outs[11], outs[13], outs[14], outs[15]
    d_w_qkv = jnp.transpose(outs[12], (0, 2, 1, 3))
    vec = [v.reshape(-1) for v in outs[:8]]
    d_b_qkv = jnp.transpose(outs[8], (1, 0, 2))
    return (outs[10][None], d_table, vec[ACC_EG], vec[ACC_EB], vec[ACC_L1G], vec[ACC_L1B],
            d_w_qkv, d_b_qkv, d_w_dense, vec[ACC_BD], vec[ACC_L2G], vec[ACC_L2B],
            d_w_fc1, outs[9].reshape(-1), d_w_fc2, vec[ACC_BF2])


def solution(mesh):
    in_specs = (P('dp', None), P('tp', None), P(None), P(None), P(None), P(None),
                P(None, 'tp', None, None), P('tp', None, None), P('tp', None), P(None),
                P(None), P(None), P(None, 'tp'), P('tp'), P('tp', None), P(None),
                P('dp', 'tp', None))
    out_specs = (P('dp', 'tp', None), P(('dp', 'tp'), None), P('dp'), P('dp'), P('dp'), P('dp'),
                 P('dp', 'tp', None, None), P(('dp', 'tp'), None, None), P(('dp', 'tp'), None), P('dp'),
                 P('dp'), P('dp'), P('dp', 'tp'), P(('dp', 'tp')), P(('dp', 'tp'), None), P('dp'))

    def run(*arrays):
        slopes = alibi_slopes(arrays[6].shape[1])
        step = functools.partial(device_step, slopes)
        mapped = jax.shard_map(step, mesh=mesh, in_specs=in_specs, out_specs=out_specs, check_vma=False)
        return mapped(*arrays)

    return run
```

```python
import functools
import jax
import jax.numpy as jnp
from jax import lax
from jax.experimental import pallas as pl
from jax.experimental.pallas import tpu as pltpu
from jax.sharding import PartitionSpec as P

EPS = 1e-5
F32 = jnp.float32
BF16 = jnp.bfloat16
VMEM = pltpu.VMEM
ANY = pl.ANY
MAX_VMEM = 67_043_328
NT_DIMS = (((1,), (1,)), ((), ()))
TN_DIMS = (((0,), (0,)), ((), ()))
GELU_A = 0.7978845608028654
GELU_B = 0.044715


def alibi_slopes(head_count):
    closest = 2 ** (head_count.bit_length() - 1)
    slope_base = 2.0 ** (-8.0 / closest)
    extra_base = 2.0 ** (-4.0 / closest)
    slopes = [slope_base ** exponent for exponent in range(1, closest + 1)]
    return slopes + [extra_base ** exponent for exponent in range(1, 2 * (head_count - closest), 2)]


def dot_nn(lhs, rhs):
    return jnp.dot(lhs, rhs, preferred_element_type=F32)


def dot_nt(lhs, rhs):
    return lax.dot_general(lhs, rhs, NT_DIMS, preferred_element_type=F32)


def dot_tn(lhs, rhs):
    return lax.dot_general(lhs, rhs, TN_DIMS, preferred_element_type=F32)


def normalize(values):
    centered = values - jnp.mean(values, axis=-1, keepdims=True)
    inv_std = lax.rsqrt(jnp.mean(centered * centered, axis=-1, keepdims=True) + EPS)
    return centered * inv_std, inv_std


def norm_backward(d_norm, x_hat, inv_std, gain_vec):
    d_hat = d_norm * gain_vec
    return inv_std * (d_hat - jnp.mean(d_hat, axis=-1, keepdims=True)
                      - x_hat * jnp.mean(d_hat * x_hat, axis=-1, keepdims=True))


def gather_kernel(ids_smem, ids_vmem, table, out, stage, rows_buf, load_sem, out_sem):
    tokens = ids_smem.shape[1]
    vocab_rows = table.shape[0]
    base = lax.axis_index('tp') * vocab_rows
    groups, group = load_sem.shape[0], tokens // load_sem.shape[0]
    span = group * 8

    @pl.loop(0, groups)
    def _(block):
        @pl.loop(0, group, unroll=8)
        def _(i):
            token = block * group + i
            row = lax.rem(ids_smem[0, token], vocab_rows)
            first = pl.multiple_of((row >> 3) << 3, 8)
            pltpu.make_async_copy(table.at[pl.ds(first, 8), :],
                                  stage.at[pl.ds(pl.multiple_of(token * 8, 8), 8), :], load_sem.at[block]).start()

    local = ids_vmem[...] - base
    inside = jnp.where(local >= 0, 1, 0) * jnp.where(local < vocab_rows, 1, 0)
    sub = jnp.where(inside > 0, local & 7, -span)
    index = lax.broadcasted_iota(jnp.int32, (span, group), 0)
    lane = lax.broadcasted_iota(jnp.int32, (span, group), 1) * 8
    copies = []
    for block in range(groups):
        pick = jnp.where(index == lane + sub[:, block * group:(block + 1) * group], 1.0, 0.0).astype(BF16)
        part = slice(block * span, (block + 1) * span)
        rows = slice(block * group, (block + 1) * group)
        pltpu.make_async_copy(table.at[pl.ds(0, span), :], stage.at[part, :], load_sem.at[block]).wait()
        rows_buf[rows, :] = dot_tn(pick, stage[part, :]).astype(BF16)
        copies.append(pltpu.make_async_copy(rows_buf.at[rows, :], out.at[rows, :], out_sem.at[block]))
        copies[-1].start()
    for copy in copies:
        copy.wait()


def gather_rows(token_ids, table):
    tokens, width = token_ids.shape[1], table.shape[1]
    groups = 8
    return pl.pallas_call(
        gather_kernel,
        out_shape=jax.ShapeDtypeStruct((tokens, width), BF16),
        in_specs=[pl.BlockSpec(memory_space=pltpu.SMEM), pl.BlockSpec(memory_space=VMEM),
                  pl.BlockSpec(memory_space=ANY)],
        out_specs=pl.BlockSpec(memory_space=ANY),
        scratch_shapes=[VMEM((tokens * 8, width), BF16), VMEM((tokens, width), BF16),
                        pltpu.SemaphoreType.DMA((groups,)), pltpu.SemaphoreType.DMA((groups,))],
        compiler_params=pltpu.CompilerParams(vmem_limit_bytes=MAX_VMEM),
        name='gather_rows',
    )(token_ids, token_ids, table)


CHUNKS = 2
ROW_STEP = 64
WIDEN_TILE = 1024
ROW_UNROLL = 1
AR_EMB, AR_DENSE, AR_DH2, AR_DH1 = range(4)
ACC_BD, ACC_L2G, ACC_L2B, ACC_BF2 = range(4)
N_COPIES = (4 * 3 + 2) * CHUNKS + 3 + 3


def step_kernel(slopes, rows_in, w_qkv, w_dense, w_fc1, w_fc2, d_out,
                emb_gain, emb_bias, ln1_gain, ln1_bias, b_qkv, b_dense, ln2_gain, ln2_bias, b_fc1, b_fc2,
                o_h1, o_h2, o_ctx, o_gelu, o_dpre, o_dqkv, o_dy, o_dr1, o_x, o_emb, o_sum, o_mine,
                y_out, o_small, o_bfc1, o_bqkv,
                wraw, wtmp, wq, wd, w1, w2, part, din, summ, cross, dy, ypart, y_in, y_send, y_cross,
                x_zero, emb, h1, qkv, ctx, r1, h2, gelu, dgelu, dpre, prob, dr1, d_kv, dqkv, bq, acc,
                send_sem, recv_sem, load_sem, out_sem):
    tp = lax.axis_index('tp')
    core = lax.rem(tp, 2)
    chip = tp // 2
    partner = tp + 1 - 2 * core
    xpeer = lax.rem(tp + 2, 4)
    seq, width = emb.shape
    size = seq // CHUNKS
    half = size // 2
    heads, head_dim = b_qkv.shape[1], b_qkv.shape[2]
    scale = head_dim ** -0.5
    hidden = heads * head_dim
    block = seq // 4

    barrier = pltpu.get_barrier_semaphore()
    for peer in (partner, xpeer):
        pl.semaphore_signal(barrier, inc=1, device_id={'tp': peer}, device_id_type=pl.DeviceIdType.MESH)

    def load(src, dst, index):
        copy = pltpu.make_async_copy(src, dst, load_sem.at[index])
        copy.start()
        return copy

    load_rows = load(rows_in, part.at[AR_EMB], 0)
    my_block = pl.ds(pl.multiple_of(tp * block, block), block)
    load_dy = load(d_out, dy.at[my_block, :], 1)
    raw_rows = wraw.shape[1]
    raw_steps = w_qkv.shape[0] // raw_rows

    def load_raw(step):
        return pltpu.make_async_copy(w_qkv.at[pl.ds(pl.multiple_of(step * raw_rows, raw_rows), raw_rows)],
                                     wraw.at[lax.rem(step, 2)], load_sem.at[6 + lax.rem(step, 2)])

    load_raw(0).start()
    load_raw(1).start()
    late_loads = [pltpu.make_async_copy(src, dst, load_sem.at[index])
                  for src, dst, index in ((w_dense, wd, 2), (w_fc2, w2, 3), (w_fc1, w1, 4))]
    load_wd, load_w2, load_w1 = late_loads

    outs = []

    def put(src, dst):
        copy = pltpu.make_async_copy(src, dst, out_sem.at[len(outs)])
        copy.start()
        outs.append(copy)

    count = [0]
    sends = []

    def remote(src, dst, peer):
        index = count[0]
        count[0] += 1
        copy = pltpu.make_async_remote_copy(src_ref=src, dst_ref=dst, send_sem=send_sem.at[index],
                                            recv_sem=recv_sem.at[index], device_id={'tp': peer},
                                            device_id_type=pl.DeviceIdType.MESH)
        sends.append(copy)
        return copy

    def at_row(start, length):
        return pl.ds(pl.multiple_of(start, half), length)

    def make_reduce(which, chunk):
        base = chunk * size
        mine, other = at_row(base + core * half, half), at_row(base + (1 - core) * half, half)
        local_in = din.at[which, pl.ds(chunk * half, half), :]
        last = which == AR_DH1
        first = remote(part.at[which, other, :], local_in, partner)
        share = remote(summ.at[which, mine, :], summ.at[which, mine, :], partner)
        if not last:
            across = remote(summ.at[which, mine, :], cross.at[which, mine, :], xpeer)
            forward = remote(cross.at[which, mine, :], cross.at[which, mine, :], partner)

        def middle():
            first.wait_recv()

            @pl.loop(0, half // 16)
            def _(i):
                rows = pl.ds(pl.multiple_of(base + core * half + i * 16, 16), 16)
                got = din[which, pl.ds(pl.multiple_of(chunk * half + i * 16, 16), 16), :]
                summ[which, rows, :] = (part[which, rows, :].astype(F32) + got.astype(F32)).astype(BF16)

            if not last:
                across.start()
            share.start()
            if last:
                put(summ.at[which, mine, :], o_mine.at[chunk * half:(chunk + 1) * half, :])

        def pass_on():
            across.wait_recv()
            forward.start()

        def finish():
            share.wait_recv()
            if not last:
                forward.wait_recv()

        return first.start, middle, pass_on, finish

    reduces = {(w, c): make_reduce(w, c) for w in range(4) for c in range(CHUNKS)}

    def ar(which, chunk, stage):
        reduces[which, chunk][stage]()

    dy_across = remote(dy.at[my_block, :], dy.at[my_block, :], xpeer)
    dy_share = remote(dy.at[my_block, :], dy.at[my_block, :], partner)
    peer_block = pl.ds(pl.multiple_of(xpeer * block, block), block)
    dy_forward = remote(dy.at[peer_block, :], dy.at[peer_block, :], partner)

    partner_block = pl.ds(pl.multiple_of(partner * block, block), block)
    far = 2 * (1 - chip) + 1 - core
    far_block = pl.ds(pl.multiple_of(far * block, block), block)
    y_near = remote(ypart.at[partner_block, :], y_in.at[0], partner)
    y_far = remote(ypart.at[far_block, :], y_in.at[1], partner)
    y_over = remote(y_send, y_cross, xpeer)

    def row_loop(chunk, body, step=ROW_STEP):
        @pl.loop(0, size // step, unroll=ROW_UNROLL)
        def _(i):
            body(pl.ds(pl.multiple_of(chunk * size + i * step, step), step))

    def chunk_rows(chunk):
        return slice(chunk * size, (chunk + 1) * size)

    def col_loop(total, tile, body, first=0):
        @pl.loop(first, total // tile)
        def _(n):
            body(pl.ds(pl.multiple_of(n * tile, tile), tile))

    def accumulate(slot, values):
        total = values[:8]
        for first in range(8, values.shape[0], 8):
            total = total + values[first:first + 8]
        acc[slot] += total

    def exchanged(which, rows):
        return summ[which, rows, :].astype(F32) + cross[which, rows, :].astype(F32)

    def unpack_qkv():
        pitch = wtmp.shape[0] // (3 * heads)
        for c in range(3):
            for h in range(heads):
                bq[0:1, c * hidden + h * head_dim:c * hidden + (h + 1) * head_dim] = b_qkv[c, h:h + 1, :]

        @pl.loop(0, raw_steps)
        def _(step):
            load_raw(step).wait()
            slot = lax.rem(step, 2)

            @pl.loop(0, raw_rows // 8)
            def _(i):
                for j in range(8):
                    for c in range(3):
                        d = i * 8 + j
                        wtmp[pl.ds(c * heads * pitch + d, heads, stride=pitch), :] = wraw[slot, d, c].astype(F32)

            @pl.when(step + 2 < raw_steps)
            def _():
                load_raw(step + 2).start()

            @pl.when(step + 3 == raw_steps)
            def _():
                for copy in late_loads:
                    copy.start()

            dst = pl.ds(pl.multiple_of(step * raw_rows, raw_rows), raw_rows)
            for c in range(3):
                for h in range(heads):
                    lo = c * hidden + h * head_dim
                    wq[dst, lo:lo + head_dim] = wtmp[(c * heads + h) * pitch:
                                                     (c * heads + h) * pitch + raw_rows, :].astype(BF16)

    def norm_first(chunk):
        def body(rows):
            values = exchanged(AR_EMB, rows)
            x_zero[rows, :] = values.astype(BF16)
            x_hat, _ = normalize(values)
            embedded = (x_hat * emb_gain[...] + emb_bias[...]).astype(BF16)
            emb[rows, :] = embedded
            e_hat, _ = normalize(embedded.astype(F32))
            h1[rows, :] = (e_hat * ln1_gain[...] + ln1_bias[...]).astype(BF16)

        row_loop(chunk, body)

    def project_qkv(chunk):
        rows = chunk_rows(chunk)

        def body(cols):
            qkv[rows, cols] = (dot_nn(h1[rows, :], wq[:, cols]) + bq[0:1, cols]).astype(BF16)

        col_loop(3 * hidden, 768, body)

    def head_cols(part_index, h):
        lo = part_index * hidden + h * head_dim
        return slice(lo, lo + head_dim)

    def attend(chunk):
        rows = chunk_rows(chunk)
        keys = (chunk + 1) * size
        row_id = lax.broadcasted_iota(jnp.int32, (size, keys), 0) + chunk * size
        col_id = lax.broadcasted_iota(jnp.int32, (size, keys), 1)
        rel = (col_id - row_id).astype(F32)
        for h in range(heads):
            slope = F32(slopes[3 * heads + h])
            for t in (2, 1, 0):
                slope = jnp.where(tp == t, F32(slopes[t * heads + h]), slope)
            scores = dot_nt(qkv[rows, head_cols(0, h)], qkv[0:keys, head_cols(1, h)]) * scale
            scores = jnp.where(col_id <= row_id, scores + slope * rel, -1e30)
            top = jnp.max(scores, axis=-1, keepdims=True)
            weight = jnp.exp(scores - top)
            p = weight / jnp.sum(weight, axis=-1, keepdims=True)
            prob[h, rows, 0:keys] = p
            ctx[rows, h * head_dim:(h + 1) * head_dim] = dot_nn(
                p.astype(BF16), qkv[0:keys, head_cols(2, h)]).astype(BF16)

    def project_dense(chunk):
        rows = chunk_rows(chunk)

        def body(cols):
            part[AR_DENSE, rows, cols] = dot_nn(ctx[rows, :], wd[:, cols]).astype(BF16)

        col_loop(width, 1024, body)

    def norm_second(chunk):
        def body(rows):
            r_one = (emb[rows, :].astype(F32) + exchanged(AR_DENSE, rows) + b_dense[...]).astype(BF16)
            r1[rows, :] = r_one
            r_hat, _ = normalize(r_one.astype(F32))
            h2[rows, :] = (r_hat * ln2_gain[...] + ln2_bias[...]).astype(BF16)

        row_loop(chunk, body)

    def gelu_grad(first, last):
        @pl.loop(first, last)
        def _(n):
            cols = pl.ds(pl.multiple_of(n * 512, 512), 512)
            dgelu[:, cols] = dot_nt(dy[...], w2[cols, :])

    def widen(chunk):
        rows = chunk_rows(chunk)

        def body(cols):
            pre = dot_nn(h2[rows, :], w1[:, cols]) + b_fc1[0:1, cols]
            square = pre * pre
            bend = jnp.tanh(GELU_A * (pre + GELU_B * (pre * square)))
            gelu[rows, cols] = (0.5 * pre * (1.0 + bend)).astype(BF16)
            slope = 0.5 * (1.0 + bend) + 0.5 * pre * (1.0 - bend * bend) * (GELU_A * (1.0 + 3.0 * GELU_B * square))
            d_pre = dgelu[rows, cols] * slope
            dpre[rows, cols] = d_pre.astype(BF16)
            total = jnp.sum(d_pre, axis=0, keepdims=True)
            o_bfc1[0:1, cols] = total if chunk == 0 else o_bfc1[0:1, cols] + total

        col_loop(w1.shape[1], WIDEN_TILE, body)

    def narrow_grad(chunk):
        rows = chunk_rows(chunk)

        def body(cols):
            part[AR_DH2, rows, cols] = dot_nt(dpre[rows, :], w1[cols, :]).astype(BF16)

        col_loop(width, 1024, body)

    def narrow(first, last):
        @pl.loop(first, last)
        def _(n):
            cols = pl.ds(pl.multiple_of(n * 512, 512), 512)
            ypart[:, cols] = dot_nn(gelu[...], w2[:, cols]).astype(BF16)

    def y_middle():
        y_near.wait_recv()
        y_far.wait_recv()

        @pl.loop(0, block // 16)
        def _(i):
            rows = pl.ds(pl.multiple_of(i * 16, 16), 16)
            src = pl.ds(pl.multiple_of(xpeer * block + i * 16, 16), 16)
            y_send[rows, :] = (ypart[src, :].astype(F32) + y_in[1, rows, :].astype(F32)).astype(BF16)

        y_over.start()

    def y_finish():
        y_over.wait_recv()

        @pl.loop(0, block // 16)
        def _(i):
            rows = pl.ds(pl.multiple_of(i * 16, 16), 16)
            src = pl.ds(pl.multiple_of(tp * block + i * 16, 16), 16)
            total = ypart[src, :].astype(F32) + y_in[0, rows, :].astype(F32) + y_cross[rows, :].astype(F32)
            y_out[rows, :] = (r1[src, :].astype(F32) + total + b_fc2[...]).astype(BF16)

    def norm_second_grad(chunk):
        def body(rows):
            r_hat, inv = normalize(r1[rows, :].astype(F32))
            d_norm = exchanged(AR_DH2, rows)
            dy_rows = dy[rows, :].astype(F32)
            grad = dy_rows + norm_backward(d_norm, r_hat, inv, ln2_gain[...])
            dr1[rows, :] = grad.astype(BF16)
            accumulate(ACC_L2G, d_norm * r_hat)
            accumulate(ACC_L2B, d_norm)
            accumulate(ACC_BD, grad)
            accumulate(ACC_BF2, dy_rows)

        row_loop(chunk, body)

    def attend_grad(chunk):
        rows = chunk_rows(chunk)
        keys = (chunk + 1) * size
        old = chunk * size
        for h in range(heads):
            cols = slice(h * head_dim, (h + 1) * head_dim)
            d_ctx = dot_nt(dr1[rows, :], wd[cols, :]).astype(BF16)
            p = prob[h, rows, 0:keys]
            d_prob = dot_nt(d_ctx, qkv[0:keys, head_cols(2, h)])
            d_score = p * (d_prob - jnp.sum(d_prob * p, axis=-1, keepdims=True))
            d_score = (d_score * scale).astype(BF16)
            d_query = dot_nn(d_score, qkv[0:keys, head_cols(1, h)])
            dqkv[rows, head_cols(0, h)] = d_query.astype(BF16)
            total = jnp.sum(d_query, axis=0, keepdims=True)
            o_bqkv[0:1, head_cols(0, h)] = total if chunk == 0 else o_bqkv[0:1, head_cols(0, h)] + total
            for index, grad in ((0, dot_tn(d_score, qkv[rows, head_cols(0, h)])),
                                (1, dot_tn(p.astype(BF16), d_ctx))):
                if old:
                    d_kv[index, 0:old, cols] += grad[:old]
                d_kv[index, old:keys, cols] = grad[old:]

    def finish_kv():
        for index in range(2):
            lo = (index + 1) * hidden
            dqkv[:, lo:lo + hidden] = d_kv[index].astype(BF16)
            o_bqkv[0:1, lo:lo + hidden] = jnp.sum(d_kv[index], axis=0, keepdims=True)

    def qkv_grad():
        def body(cols):
            part[AR_DH1, :, cols] = dot_nt(dqkv[...], wq[cols, :]).astype(BF16)

        col_loop(width, 1024, body)

    START, MIDDLE, PASS, FINISH = range(4)
    acc[...] = jnp.zeros_like(acc)
    load_rows.wait()
    pl.semaphore_wait(barrier, 2)
    ar(AR_EMB, 0, START)
    ar(AR_EMB, 1, START)
    ar(AR_EMB, 0, MIDDLE)
    ar(AR_EMB, 1, MIDDLE)
    load_dy.wait()
    dy_across.start()
    dy_share.start()
    unpack_qkv()
    load_wd.wait()
    ar(AR_EMB, 0, PASS)
    ar(AR_EMB, 0, FINISH)
    norm_first(0)
    project_qkv(0)
    ar(AR_EMB, 1, PASS)
    attend(0)
    project_dense(0)
    ar(AR_DENSE, 0, START)
    ar(AR_EMB, 1, FINISH)
    norm_first(1)
    put(h1, o_h1)
    put(x_zero, o_x)
    put(emb, o_emb)
    ar(AR_DENSE, 0, MIDDLE)
    project_qkv(1)
    dy_across.wait_recv()
    dy_forward.start()
    attend(1)
    put(ctx, o_ctx)
    project_dense(1)
    ar(AR_DENSE, 1, START)
    dy_share.wait_recv()
    dy_forward.wait_recv()
    put(dy, o_dy)
    load_w2.wait()
    gelu_grad(0, 1)
    ar(AR_DENSE, 1, MIDDLE)
    gelu_grad(1, 4)
    ar(AR_DENSE, 0, PASS)
    ar(AR_DENSE, 0, FINISH)
    load_w1.wait()
    norm_second(0)
    widen(0)
    narrow_grad(0)
    ar(AR_DENSE, 1, PASS)
    ar(AR_DH2, 0, START)
    ar(AR_DENSE, 1, FINISH)
    norm_second(1)
    put(h2, o_h2)
    ar(AR_DH2, 0, MIDDLE)
    widen(1)
    put(gelu, o_gelu)
    put(dpre, o_dpre)
    narrow_grad(1)
    ar(AR_DH2, 1, START)
    narrow(0, 2)
    ar(AR_DH2, 1, MIDDLE)
    ar(AR_DH2, 0, PASS)
    narrow(2, 4)
    y_near.start()
    y_far.start()
    ar(AR_DH2, 0, FINISH)
    norm_second_grad(0)
    y_middle()
    attend_grad(0)
    ar(AR_DH2, 1, PASS)
    ar(AR_DH2, 1, FINISH)
    norm_second_grad(1)
    put(dr1, o_dr1)
    attend_grad(1)
    finish_kv()
    put(dqkv, o_dqkv)
    qkv_grad()
    ar(AR_DH1, 0, START)
    ar(AR_DH1, 1, START)
    y_finish()
    ar(AR_DH1, 0, MIDDLE)
    ar(AR_DH1, 1, MIDDLE)
    ar(AR_DH1, 0, FINISH)
    ar(AR_DH1, 1, FINISH)
    put(summ.at[AR_DH1], o_sum)
    for slot in range(4):
        o_small[slot:slot + 1, :] = jnp.sum(acc[slot], axis=0, keepdims=True)
    for copy in sends:
        copy.wait_send()
    for copy in outs:
        copy.wait()


def run_step(slopes, rows, w_qkv, w_dense, w_fc1, w_fc2, d_out, vectors, b_qkv):
    seq, width = rows.shape
    ffn = w_fc1.shape[1]
    hidden = w_dense.shape[0]
    heads, head_dim = w_qkv.shape[2], w_qkv.shape[3]
    block = seq // 4
    (emb_gain, emb_bias, ln1_gain, ln1_bias, b_dense, ln2_gain, ln2_bias, b_fc1, b_fc2) = vectors
    shape = jax.ShapeDtypeStruct
    any_spec = pl.BlockSpec(memory_space=ANY)
    vmem_spec = pl.BlockSpec(memory_space=VMEM)
    raw_rows = 256
    pitch = raw_rows + 8
    out_shapes = ([shape((seq, n), BF16) for n in (width, width, hidden, ffn, ffn, 3 * hidden, width, width, width,
                                                   width, width)]
                  + [shape((seq // 2, width), BF16), shape((block, width), BF16), shape((4, width), F32), shape((1, ffn), F32),
                     shape((1, 3 * hidden), F32)])
    scratch = [VMEM((2, raw_rows, 3, heads, head_dim), BF16), VMEM((3 * heads * pitch, head_dim), F32),
               VMEM((width, 3 * hidden), BF16), VMEM((hidden, width), BF16), VMEM((width, ffn), BF16),
               VMEM((ffn, width), BF16),
               VMEM((4, seq, width), BF16), VMEM((4, seq // 2, width), BF16), VMEM((4, seq, width), BF16),
               VMEM((3, seq, width), BF16), VMEM((seq, width), BF16),
               VMEM((seq, width), BF16), VMEM((2, block, width), BF16), VMEM((block, width), BF16),
               VMEM((block, width), BF16),
               VMEM((seq, width), BF16),
               VMEM((seq, width), BF16), VMEM((seq, width), BF16), VMEM((seq, 3 * hidden), BF16),
               VMEM((seq, hidden), BF16), VMEM((seq, width), BF16), VMEM((seq, width), BF16),
               VMEM((seq, ffn), BF16), VMEM((seq, ffn), F32), VMEM((seq, ffn), BF16),
               VMEM((heads, seq, seq), F32), VMEM((seq, width), BF16), VMEM((2, seq, hidden), F32),
               VMEM((seq, 3 * hidden), BF16), VMEM((1, 3 * hidden), F32),
               VMEM((4, 8, width), F32),
               pltpu.SemaphoreType.DMA((N_COPIES,)), pltpu.SemaphoreType.DMA((N_COPIES,)),
               pltpu.SemaphoreType.DMA((8,)), pltpu.SemaphoreType.DMA((13,))]
    return pl.pallas_call(
        functools.partial(step_kernel, slopes),
        out_shape=out_shapes,
        in_specs=[any_spec] * 6 + [vmem_spec] * 10,
        out_specs=[any_spec] * 12 + [vmem_spec] * 4,
        scratch_shapes=scratch,
        compiler_params=pltpu.CompilerParams(collective_id=0, has_side_effects=True, vmem_limit_bytes=MAX_VMEM),
        name='block_step',
    )(rows, w_qkv, w_dense, w_fc1, w_fc2, d_out, emb_gain, emb_bias, ln1_gain, ln1_bias, b_qkv, b_dense,
      ln2_gain, ln2_bias, b_fc1, b_fc2)


TABLE_TILE = 1024
WEIGHT_TILE = 1024
QKV_TILE = 256


def grads_kernel(small, bqkv, bfc1, y_part, h1_in, h2_in, ctx_in, gelu_in, dpre_in, dqkv_in, dy_in, dr1_in, *refs):
    vec_out, (o_bqkv, o_bfc1, o_y, o_qkv, o_dense, o_fc1, o_fc2) = refs[:4], refs[4:11]
    (h1, h2, ctx, gelu, dpre, dqkv, dy, dr1, weight_ring, qkv_ring, tmp,
     load_sem, weight_sem, qkv_sem, y_sem) = refs[11:]
    _, heads, head_dim = o_bqkv.shape
    width = h1.shape[1]
    loads = []
    for index, (src, dst) in enumerate(((h2_in, h2), (dpre_in, dpre), (gelu_in, gelu), (dy_in, dy),
                                        (h1_in, h1), (dqkv_in, dqkv), (ctx_in, ctx), (dr1_in, dr1))):
        loads.append(pltpu.make_async_copy(src, dst, load_sem.at[index]))
        loads[index].start()
    copy_y = pltpu.make_async_copy(y_part, o_y, y_sem)
    copy_y.start()
    for slot in range(4):
        vec_out[slot][...] = small[slot:slot + 1, :]
    for c in range(3):
        for h in range(heads):
            lo = (c * heads + h) * head_dim
            o_bqkv[c, h:h + 1, :] = bqkv[0:1, lo:lo + head_dim]
    o_bfc1[...] = bfc1[...]
    pitch = tmp.shape[0] // (3 * heads)

    def qkv_copy(step, slot):
        return pltpu.make_async_copy(
            qkv_ring.at[slot], o_qkv.at[pl.ds(pl.multiple_of(step * QKV_TILE, QKV_TILE), QKV_TILE)],
            qkv_sem.at[slot])

    def qkv_step(step, slot):
        cols = pl.ds(pl.multiple_of(step * QKV_TILE, QKV_TILE), QKV_TILE)
        grad = dot_tn(h1[:, cols], dqkv[...])
        for index in range(3 * heads):
            tmp[index * pitch:index * pitch + QKV_TILE, :] = grad[:, index * head_dim:(index + 1) * head_dim]

        @pl.loop(0, QKV_TILE // 32)
        def _(i):
            for j in range(32):
                for c in range(3):
                    d = i * 32 + j
                    qkv_ring[slot, d, c] = tmp[pl.ds(c * heads * pitch + d, heads, stride=pitch), :].astype(BF16)

        qkv_copy(step, slot).start()

    pending = {}
    order = []
    for lhs, rhs, out, needs in ((h2, dpre, o_fc1, (0, 1)), (gelu, dy, o_fc2, (2, 3)), (ctx, dr1, o_dense, (6, 7))):
        tile = min(WEIGHT_TILE, lhs.shape[1])
        for step in range(lhs.shape[1] // tile):
            order.append((lhs, rhs, out, needs if step == 0 else (), step * tile, tile))
    for index, (lhs, rhs, out, needs, lo, tile) in enumerate(order):
        slot = index % 2
        for load in needs:
            loads[load].wait()
        if slot in pending:
            pending[slot].wait()
        weight_ring[slot, 0:tile, :] = dot_tn(lhs[:, lo:lo + tile], rhs[...]).astype(BF16)
        pending[slot] = pltpu.make_async_copy(weight_ring.at[slot, 0:tile, :], out.at[lo:lo + tile, :],
                                              weight_sem.at[slot])
        pending[slot].start()

    loads[4].wait()
    loads[5].wait()
    qkv_steps = width // QKV_TILE

    @pl.loop(0, qkv_steps)
    def _(step):
        slot = lax.rem(step, 2)

        @pl.when(step >= 2)
        def _():
            qkv_copy(step - 2, slot).wait()

        qkv_step(step, slot)

    for step in range(qkv_steps - 2, qkv_steps):
        qkv_copy(step, step % 2).wait()
    for copy in pending.values():
        copy.wait()
    copy_y.wait()


def all_grads(heads, head_dim, small, bqkv, bfc1, y_part, acts):
    shape = jax.ShapeDtypeStruct
    tokens, width = acts[0].shape
    ffn, hidden = acts[3].shape[1], heads * head_dim
    vmem_spec, any_spec = pl.BlockSpec(memory_space=VMEM), pl.BlockSpec(memory_space=ANY)
    return pl.pallas_call(
        grads_kernel,
        out_shape=[shape((1, width), F32)] * 4 + [
            shape((3, heads, head_dim), F32), shape(bfc1.shape, F32), shape(y_part.shape, BF16),
            shape((width, 3, heads, head_dim), BF16), shape((hidden, width), BF16),
            shape((width, ffn), BF16), shape((ffn, width), BF16)],
        in_specs=[vmem_spec] * 3 + [any_spec] * 9,
        out_specs=[vmem_spec] * 6 + [any_spec] * 5,
        scratch_shapes=[VMEM(a.shape, BF16) for a in acts] + [
            VMEM((2, WEIGHT_TILE, width), BF16),
            VMEM((2, QKV_TILE, 3, heads, head_dim), BF16), VMEM((3 * heads * (QKV_TILE + 8), head_dim), F32),
            pltpu.SemaphoreType.DMA((len(acts),)), pltpu.SemaphoreType.DMA((2,)),
            pltpu.SemaphoreType.DMA((2,)), pltpu.SemaphoreType.DMA],
        compiler_params=pltpu.CompilerParams(vmem_limit_bytes=MAX_VMEM),
        cost_estimate=pl.CostEstimate(flops=2 * tokens * width * (2 * ffn + 4 * hidden), transcendentals=0,
                                      bytes_accessed=2 * width * (2 * ffn + 4 * hidden)),
        name='all_grads',
    )(small, bqkv, bfc1, y_part, *acts)


def table_kernel(ids, ln1_gain, emb_gain, sum_in, mine_in, other_in, dr1_in, x_in, emb_in, *refs):
    vec_out, o_table = refs[:4], refs[4]
    sums, mine, other, dr1, x_zero, emb, dx, acc, ring, load_sem, table_sem = refs[5:]
    tokens, _ = dx.shape
    vocab_rows = o_table.shape[0]
    tp = lax.axis_index('tp')
    core = lax.rem(tp, 2)
    half = tokens // CHUNKS // 2
    loads = [pltpu.make_async_copy(src, dst, load_sem.at[index]) for index, (src, dst) in enumerate(
        ((sum_in, sums), (mine_in, mine), (other_in, other), (dr1_in, dr1), (x_in, x_zero), (emb_in, emb)))]
    for copy in loads:
        copy.start()
    acc[...] = jnp.zeros_like(acc)
    for copy in loads:
        copy.wait()

    def accumulate(slot, values):
        total = values[:8]
        for first in range(8, values.shape[0], 8):
            total = total + values[first:first + 8]
        acc[slot] += total

    @pl.loop(0, CHUNKS * 2)
    def _(i):
        chunk, owned = i // 2, 1 - lax.rem(i, 2)
        source = pl.ds(pl.multiple_of(chunk * half, half), half)
        place = core * owned + (1 - core) * (1 - owned)
        rows = pl.ds(pl.multiple_of((chunk * 2 + place) * half, half), half)
        got = jnp.where(owned == 1, mine[source, :].astype(F32), other[source, :].astype(F32))
        d_norm = sums[rows, :].astype(F32) + got
        e_hat, e_inv = normalize(emb[rows, :].astype(F32))
        grad = dr1[rows, :].astype(F32) + norm_backward(d_norm, e_hat, e_inv, ln1_gain[...])
        accumulate(2, d_norm * e_hat)
        accumulate(3, d_norm)
        x_hat, x_inv = normalize(x_zero[rows, :].astype(F32))
        accumulate(0, grad * x_hat)
        accumulate(1, grad)
        dx[rows, :] = norm_backward(grad, x_hat, x_inv, emb_gain[...]).astype(BF16)

    first_row = tp * vocab_rows

    def table_copy(step):
        slot = lax.rem(step, 2)
        return pltpu.make_async_copy(
            ring.at[slot], o_table.at[pl.ds(pl.multiple_of(step * TABLE_TILE, TABLE_TILE), TABLE_TILE), :],
            table_sem.at[slot])

    @pl.loop(0, vocab_rows // TABLE_TILE)
    def _(step):
        @pl.when(step >= 2)
        def _():
            table_copy(step - 2).wait()

        row_id = lax.broadcasted_iota(jnp.int32, (TABLE_TILE, tokens), 0) + (first_row + step * TABLE_TILE)
        pick = jnp.where(row_id == ids[...], 1.0, 0.0).astype(BF16)
        ring[lax.rem(step, 2)] = dot_nn(pick, dx[...])
        table_copy(step).start()

    for slot in range(4):
        vec_out[slot][...] = jnp.sum(acc[slot], axis=0, keepdims=True)
    for step in range(vocab_rows // TABLE_TILE - 2, vocab_rows // TABLE_TILE):
        table_copy(step).wait()


def table_grads(token_ids, vocab_rows, ln1_gain, emb_gain, sums, mine, other, dr1, x_zero, emb):
    shape = jax.ShapeDtypeStruct
    tokens, width = emb.shape
    vmem_spec, any_spec = pl.BlockSpec(memory_space=VMEM), pl.BlockSpec(memory_space=ANY)
    full = VMEM((tokens, width), BF16)
    part = VMEM((tokens // 2, width), BF16)
    return pl.pallas_call(
        table_kernel,
        out_shape=[shape((1, width), F32)] * 4 + [shape((vocab_rows, width), F32)],
        in_specs=[vmem_spec] * 3 + [any_spec] * 6,
        out_specs=[vmem_spec] * 4 + [any_spec],
        scratch_shapes=[full, part, part, full, full, full, full, VMEM((4, 8, width), F32),
                        VMEM((2, TABLE_TILE, width), F32),
                        pltpu.SemaphoreType.DMA((6,)), pltpu.SemaphoreType.DMA((2,))],
        compiler_params=pltpu.CompilerParams(vmem_limit_bytes=MAX_VMEM),
        cost_estimate=pl.CostEstimate(flops=2 * tokens * width * vocab_rows, transcendentals=0,
                                      bytes_accessed=4 * width * vocab_rows),
        name='table_grads',
    )(token_ids, ln1_gain, emb_gain, sums, mine, other, dr1, x_zero, emb)


def device_step(slopes, token_ids, embed_table, emb_gain, emb_bias, ln1_gain, ln1_bias,
                w_qkv, b_qkv, w_dense, b_dense, ln2_gain, ln2_bias,
                w_fc1, b_fc1, w_fc2, b_fc2, d_out):
    heads, head_dim = w_qkv.shape[1], w_qkv.shape[3]
    rows = gather_rows(token_ids, embed_table)
    vectors = [v.reshape(1, -1) for v in (emb_gain, emb_bias, ln1_gain, ln1_bias, b_dense, ln2_gain, ln2_bias,
                                          b_fc1, b_fc2)]
    (h1, h2, ctx, gelu, dpre, dqkv, dy, dr1, x_zero, emb, sums, own, y_part, small, bfc1, bqkv) = run_step(
        slopes, rows, jnp.transpose(w_qkv, (0, 2, 1, 3)), w_dense, w_fc1, w_fc2, d_out[0], vectors,
        jnp.transpose(b_qkv, (1, 0, 2)))
    mine = lax.ppermute(own, 'tp', ((0, 2), (2, 0), (1, 3), (3, 1)))
    outs = all_grads(heads, head_dim, small, bqkv, bfc1, y_part, (h1, h2, ctx, gelu, dpre, dqkv, dy, dr1))
    other = lax.ppermute(mine, 'tp', ((0, 1), (1, 0), (2, 3), (3, 2)))
    last = table_grads(token_ids, embed_table.shape[0], vectors[2], vectors[0], sums, mine, other, dr1, x_zero, emb)
    d_emb_gain, d_emb_bias, d_ln1_gain, d_ln1_bias = [v.reshape(-1) for v in last[:4]]
    vec = [v.reshape(-1) for v in outs[:4]]
    d_b_qkv = jnp.transpose(outs[4], (1, 0, 2))
    d_w_qkv = jnp.transpose(outs[7], (0, 2, 1, 3))
    return (outs[6][None], last[4], d_emb_gain, d_emb_bias, d_ln1_gain, d_ln1_bias,
            d_w_qkv, d_b_qkv, outs[8], vec[ACC_BD], vec[ACC_L2G], vec[ACC_L2B],
            outs[9], outs[5].reshape(-1), outs[10], vec[ACC_BF2])


def solution(mesh):
    in_specs = (P('dp', None), P('tp', None), P(None), P(None), P(None), P(None),
                P(None, 'tp', None, None), P('tp', None, None), P('tp', None), P(None),
                P(None), P(None), P(None, 'tp'), P('tp'), P('tp', None), P(None),
                P('dp', 'tp', None))
    out_specs = (P('dp', 'tp', None), P(('dp', 'tp'), None), P('dp'), P('dp'), P('dp'), P('dp'),
                 P('dp', 'tp', None, None), P(('dp', 'tp'), None, None), P(('dp', 'tp'), None), P('dp'),
                 P('dp'), P('dp'), P('dp', 'tp'), P(('dp', 'tp')), P(('dp', 'tp'), None), P('dp'))

    def run(*arrays):
        slopes = alibi_slopes(arrays[6].shape[1])
        step = functools.partial(device_step, slopes)
        mapped = jax.shard_map(step, mesh=mesh, in_specs=in_specs, out_specs=out_specs, check_vma=False)
        return mapped(*arrays)

    return run
```
